768 devices in a mesh: gx: 96 (over y, z), gy: 8 (over x, core).
Axes of the slice: x: 4, y: 8, z: 12, core: 2. Of those that a mesh axis runs over, the one named last changes fastest.
Arguments:
- ice_rhs: float32 [2, 6144, 2048], P(None, 'gx', 'gy'), may hold values from -18.6 to 18.6
- ice_guess: float32 [2, 6144, 2048], P(None, 'gx', 'gy'), may hold values from -9.3 to 9.3
- ocean_rhs: float32 [6144, 2048], P('gx', 'gy'), may hold values from -18.6 to 18.6
- ocean_guess: float32 [6144, 2048], P('gx', 'gy'), may hold values from -9.3 to 9.3
- ice_diag: float32 [6144, 2048], P('gx', 'gy'), may hold values from 1 to 4
- ice_visc: float32 [6144, 2048], P('gx', 'gy'), may hold values from 0.5 to 1.5
- coriolis: float32 [6144, 2048], P('gx', 'gy'), may hold values from -1.5 to 1.5
- depth_factor: float32 [6144, 2048], P('gx', 'gy'), may hold values from 1 to 3
- wet_mask: int32 [6144, 2048], P('gx', 'gy'), may hold values 0 or 1
- ice_mask: int32 [6144, 2048], P('gx', 'gy'), may hold values from 0 to 1, as said below
Outputs:
- ice_velocity: float32 [2, 6144, 2048], P(None, 'gx', 'gy')
- ocean_level: float32 [6144, 2048], P('gx', 'gy')
The draws below stay inside these ranges and needn't reach their ends.
Inputs may be any that keep to these rules, and one draw needn't show every extreme that they name: `ice_mask`: 1 where sea ice covers the cell.
All inputs are finite; a program needn't handle non-finite values. No bound on the sum of `wet_mask` on one device may be relied on, other than what follows from the above.
Results may differ from the reference program's by a relative error of at most 0.00005.
Values sent between devices are 32-bit elements; how exact they have to be, the bound alone decides.
A program may use at most 32 MiB of HBM per device.

```python
import math
import jax
import jax.numpy as jnp
from jax import lax

NX = 6144
NY = 2048


def draw_ice_mask(key, part):
    rows = lax.broadcasted_iota(jnp.int32, (NX, NY), 1)
    polar = jnp.logical_or(rows * 8 >= 5 * NY, rows * 8 < 2 * NY)
    limit = jnp.where(polar, 85, 6)
    rolled = jax.random.randint(jax.random.fold_in(key, 17), (NX, NY), 0, 100)
    return (rolled < limit).astype(jnp.int32)


def northern_field(key, shape, scale):
    rows = lax.broadcasted_iota(jnp.int32, shape, len(shape) - 1).astype(jnp.float32)
    envelope = 0.1 + 3.0 * jnp.exp(-(NY - 1 - rows) / 32.0)
    noise = jnp.clip(jax.random.normal(key, shape, jnp.float32), -6.0, 6.0)
    return (scale * noise * envelope).astype(jnp.float32)


def draw_ice_rhs(key, part):
    return northern_field(jax.random.fold_in(key, 101), (2, NX, NY), 1.0)


def draw_ice_guess(key, part):
    return northern_field(jax.random.fold_in(key, 202), (2, NX, NY), 0.5)


def draw_ocean_rhs(key, part):
    return northern_field(jax.random.fold_in(key, 303), (NX, NY), 1.0)


def draw_ocean_guess(key, part):
    return northern_field(jax.random.fold_in(key, 404), (NX, NY), 0.5)


def plant(values, rng, smallest, high):
    longest = values.shape.index(max(values.shape))
    spots = []
    for shift in (0, 1):
        where = [jax.random.randint(jax.random.fold_in(rng, axis), (), 0, length) for axis, length in enumerate(values.shape)]
        where[longest] = (where[longest] + shift) % values.shape[longest]
        spots.append(tuple(where))
    return values.at[spots[0]].set(smallest).at[spots[1]].set(high)


def shard_levels(stream_key, dims, shards, low, high):
    def one(position, blocks):
        draws = jax.random.uniform(jax.random.fold_in(jax.random.fold_in(stream_key, 6), position), (blocks,), jnp.float32, low / len(shards), high / len(shards))
        return jnp.repeat(jnp.exp(draws), dims[position] // blocks).reshape((-1,) + (1,) * (len(dims) - position - 1))

    level = one(*shards[0])
    for cut in shards[1:]:
        level = level * one(*cut)
    return level


def setup_inputs(seed: int = 0) -> dict:
    streams_of = jax.random.split(jax.random.key(seed), 11)
    return {
        "ice_rhs": draw_ice_rhs(jax.random.fold_in(streams_of[10], 71), 0),
        "ice_guess": draw_ice_guess(jax.random.fold_in(streams_of[10], 71), 0),
        "ocean_rhs": draw_ocean_rhs(jax.random.fold_in(streams_of[10], 71), 0),
        "ocean_guess": draw_ocean_guess(jax.random.fold_in(streams_of[10], 71), 0),
        "ice_diag": jnp.clip(jnp.exp(math.log(4.0) - 1.3862944 * jax.random.uniform(streams_of[4], (NX, NY), jnp.float32) ** shard_levels(streams_of[4], (NX, NY), ((0, 96), (1, 8)), -0.2, 0.2)), 1.0, 4.0),
        "ice_visc": jnp.clip(jnp.exp(math.log(1.5) - 1.0986123 * jax.random.uniform(streams_of[5], (NX, NY), jnp.float32) ** shard_levels(streams_of[5], (NX, NY), ((0, 96), (1, 8)), -0.2, 0.2)), 0.5, 1.5),
        "coriolis": jnp.clip(jax.random.uniform(streams_of[6], (NX, NY), jnp.float32, -1.5, 1.5) * shard_levels(streams_of[6], (NX, NY), ((0, 96), (1, 8)), -0.4, 0.0), -1.5, 1.5),
        "depth_factor": jnp.clip(jnp.exp(math.log(3.0) - 1.0986123 * jax.random.uniform(streams_of[7], (NX, NY), jnp.float32) ** shard_levels(streams_of[7], (NX, NY), ((0, 96), (1, 8)), -0.2, 0.2)), 1.0, 3.0),
        "wet_mask": plant((jax.random.randint(streams_of[8], (NX, NY), 0, 5) < 4).astype(jnp.int32), jax.random.fold_in(streams_of[8], 1), 0, 1),
        "ice_mask": draw_ice_mask(jax.random.fold_in(streams_of[10], 71), 0),
    }


def neighbours(q):
    signs = jnp.array([-1.0, -1.0, 1.0], jnp.float32)[:, None]
    east = jnp.roll(q, -1, axis=1)
    west = jnp.roll(q, 1, axis=1)
    ghost = signs * q[:, ::-1, -1]
    north = jnp.concatenate([q[:, :, 1:], ghost[:, :, None]], axis=2)
    south = jnp.concatenate([jnp.zeros_like(q[:, :, :1]), q[:, :, :-1]], axis=2)
    return east + west + north + south

def operate(field, act, root, diag, coriolis):
    q = act * root * field
    lap = 4.0 * q - neighbours(q)
    turn = jnp.stack([-coriolis * field[1], coriolis * field[0], jnp.zeros_like(coriolis)])
    return act * (diag * field + root * lap + turn) + (1.0 - act) * field

def reference(ice_rhs, ice_guess, ocean_rhs, ocean_guess, ice_diag, ice_visc, coriolis, depth_factor, wet_mask, ice_mask):
    wet = wet_mask.astype(jnp.float32)
    active = wet * ice_mask.astype(jnp.float32)
    act = jnp.stack([active, active, wet])
    root = jnp.stack([ice_visc, ice_visc, depth_factor])
    diag = jnp.stack([ice_diag, ice_diag, jnp.ones_like(ice_diag)])
    inverse = 1.0 / (act * (diag + 4.0 * root * root) + 1.0 - act)

    def apply(ice_part, ocean_part):
        out = operate(jnp.concatenate([ice_part, ocean_part[None]]), act, root, diag, coriolis)
        return (out[:2], out[2])
    ice_start, ocean_start = apply(ice_guess, ocean_guess)
    r = ice_rhs - ice_start
    ro = ocean_rhs - ocean_start
    beta = jnp.sqrt(jnp.sum(r * r))
    v1 = r / beta
    z1 = inverse[:2] * v1
    z0 = inverse[2] * ro
    w1, ap0 = apply(z1, z0)
    h11 = jnp.sum(w1 * v1)
    other = w1 - h11 * v1
    h21 = jnp.sqrt(jnp.sum(other * other))
    v2 = other / h21
    z2 = inverse[:2] * v2
    rz0 = jnp.sum(ro * z0)
    alpha0 = rz0 / jnp.sum(z0 * ap0)
    level = ocean_guess + alpha0 * z0
    ro1 = ro - alpha0 * ap0
    zn = inverse[2] * ro1
    rz1 = jnp.sum(ro1 * zn)
    p1 = zn + rz1 / rz0 * z0
    w2, ap1 = apply(z2, p1)
    alpha1 = rz1 / jnp.sum(p1 * ap1)
    level = level + alpha1 * p1
    h12 = jnp.sum(w2 * v1)
    h22 = jnp.sum(w2 * v2)
    rest = w2 - h12 * v1 - h22 * v2
    h32sq = jnp.sum(rest * rest)
    g11 = h11 * h11 + h21 * h21
    g12 = h11 * h12 + h21 * h22
    g22 = h12 * h12 + h22 * h22 + h32sq
    first_rhs = beta * h11
    second_rhs = beta * h12
    det = g11 * g22 - g12 * g12
    y_first = (g22 * first_rhs - g12 * second_rhs) / det
    y_second = (g11 * second_rhs - g12 * first_rhs) / det
    velocity = ice_guess + y_first * z1 + y_second * z2
    return (velocity, level)
```

```python
import functools

import jax
import jax.numpy as jnp
from jax import lax
from jax.experimental import pallas as pl
from jax.experimental.pallas import tpu as pltpu
from jax.sharding import PartitionSpec as P

MESH = pl.DeviceIdType.MESH

M_U, M_V, H_U, H_V, M_O, H_O, B_I, B_O, TURN = range(9)
GROUPS = ((M_U, M_V, H_U, H_V, M_O), (H_O, B_I, B_O, TURN))
PACK = 48
ROWS = 64
COLS = 256
EXT_ROWS = ROWS + 8
EXT_COLS = COLS + 128


def iota(shape, dim):
    return lax.broadcasted_iota(jnp.int32, shape, dim)


def around(q):
    rows, cols = q.shape
    return (
        pltpu.roll(q, 1, 0) + pltpu.roll(q, rows - 1, 0) + pltpu.roll(q, 1, 1) + pltpu.roll(q, cols - 1, 1)
    )


def inner_block(x):
    return x[:ROWS, :COLS]


def kernel(
    sizes,
    ice_rhs,
    ice_guess,
    ocean_rhs,
    ocean_guess,
    ice_diag,
    ice_visc,
    coriolis,
    depth_factor,
    wet_mask,
    ice_mask,
    velocity,
    level,
    v_rhs,
    v_guess,
    v_orhs,
    v_oguess,
    v_diag,
    v_visc,
    v_cor,
    v_depth,
    v_wet,
    v_ice,
    fields,
    local,
    zonal_out,
    zonal_in,
    merid_out,
    merid_in,
    sum_gy,
    sum_z,
    sum_y,
    load_sems,
    halo_send,
    halo_recv,
    gy_send,
    gy_recv,
    z_send,
    z_recv,
    y_send,
    y_recv,
):
    ny, nz, ngy = sizes
    ngx = ny * nz
    gx = lax.axis_index("gx")
    gy = lax.axis_index("gy")
    yy = gx // nz
    zz = lax.rem(gx, nz)
    top = gy == ngy - 1
    bottom = gy == 0

    loads = []
    for i, (src, dst) in enumerate(
        (
            (ice_rhs, v_rhs),
            (ice_guess, v_guess),
            (ocean_rhs, v_orhs),
            (ocean_guess, v_oguess),
            (ice_diag, v_diag),
            (ice_visc, v_visc),
            (coriolis, v_cor),
            (depth_factor, v_depth),
            (wet_mask, v_wet),
            (ice_mask, v_ice),
        )
    ):
        loads.append(pltpu.make_async_copy(src, dst, load_sems.at[i]))

    def wrap(x):
        return lax.rem(x + ngx, ngx)

    def north_of(step):
        there = wrap(gx + step)
        return jnp.where(top, ngx - 1 - there, there), jnp.where(top, gy, gy + 1)

    def south_of(step):
        return wrap(gx + step), jnp.where(bottom, gy, gy - 1)

    east = (wrap(gx + 1), gy)
    west = (wrap(gx - 1), gy)
    norths = [north_of(step) for step in (0, 1, -1)]
    souths = [south_of(step) for step in (0, 1, -1)]
    gy_peers = [lax.rem(gy + d, ngy) for d in range(1, ngy)]
    z_peers = [lax.rem(zz + d, nz) for d in range(1, nz)]
    y_peers = [lax.rem(yy + d, ny) for d in range(1, ny)]

    barrier = pltpu.get_barrier_semaphore()

    def greet(device):
        pl.semaphore_signal(barrier, inc=1, device_id=device, device_id_type=MESH)

    mirror_self = [jnp.logical_and(top, norths[k][0] == gx) for k in (1, 2)]

    greet(norths[0])
    for k in (1, 2):

        @pl.when(jnp.logical_not(mirror_self[k - 1]))
        def _():
            greet(norths[k])

    for p in z_peers:
        greet((yy * nz + p, gy))
    for p in y_peers:
        greet((p * nz + zz, gy))
    for p in gy_peers:
        greet((gx, p))
    greet(east)
    greet(west)

    @pl.when(jnp.logical_not(bottom))
    def _():
        for device in souths:
            greet(device)

    for copy in loads:
        copy.start()
    for copy in loads:
        copy.wait()

    wet = v_wet[...].astype(jnp.float32)
    active = wet * v_ice[...].astype(jnp.float32)
    visc = v_visc[...]
    depth = v_depth[...]
    d_i = active * (v_diag[...] + 4.0 * visc * visc) + 1.0 - active
    d_o = wet * (1.0 + 4.0 * depth * depth) + 1.0 - wet
    p_i = 1.0 / d_i
    p_o = 1.0 / d_o
    r_i = active * visc
    r_o = wet * depth
    s_i = r_i * p_i
    s_o = r_o * p_o
    c = active * v_cor[...]
    g_u = v_guess[0]
    g_v = v_guess[1]
    g_o = v_oguess[...]
    h_u = v_rhs[0] - d_i * g_u + c * g_v
    h_v = v_rhs[1] - d_i * g_v - c * g_u
    h_o = v_orhs[...] - d_o * g_o
    own = {
        M_U: r_i * g_u,
        M_V: r_i * g_v,
        M_O: r_o * g_o,
        H_U: s_i * h_u,
        H_V: s_i * h_v,
        H_O: s_o * h_o,
        B_I: r_i * s_i,
        B_O: r_o * s_o,
        TURN: c * p_i,
    }
    for k, value in enumerate((h_u, h_v, h_o, r_i, r_o, p_i, p_o)):
        local[k] = value
    for f in range(9):
        fields[f, 0:ROWS, 0:COLS] = own[f]

    sub = iota((8, COLS), 0)
    for t in range(5):
        a, b = 2 * t, min(2 * t + 1, 8)
        first_a, last_a = own[a][0:8], own[a][ROWS - 8 : ROWS]
        first_b, last_b = own[b][0:8], own[b][ROWS - 8 : ROWS]
        zonal_out[0, t] = jnp.where(sub >= 4, last_a, pltpu.roll(last_b, 3, 0))
        zonal_out[1, t] = jnp.where(sub < 4, first_a, pltpu.roll(first_b, 5, 0))

    lane = iota((ROWS, 128), 1)
    halves = []
    for group in GROUPS:
        packed = jnp.zeros((ROWS, 128), jnp.float32)
        for k, f in enumerate(group):
            edge = jnp.where(lane < 64, own[f][:, 0:128], own[f][:, COLS - 128 : COLS])
            moved = pltpu.roll(edge, 8 * (k + 1), 1)
            packed = jnp.where(jnp.logical_and(lane >= 8 * k + 4, lane < 8 * k + 12), moved, packed)
        halves.append(packed)
    turned = jnp.transpose(jnp.concatenate(halves, axis=0))[0:PACK]
    merid_out[0] = turned
    merid_out[1] = turned

    @pl.when(top)
    def _():
        row = iota((PACK, 128), 0)
        within = lax.rem(row, 8)
        flipped = jnp.where(
            within == 0,
            pltpu.roll(turned, 1, 0),
            jnp.where(within == 1, pltpu.roll(turned, 3, 0), pltpu.roll(turned, 5, 0)),
        )
        swap = jnp.where(
            (iota((128, 128), 0) ^ iota((128, 128), 1)) == 63, 1.0, 0.0
        ).astype(jnp.float32)
        mirrored = jnp.dot(
            flipped, swap, precision=lax.Precision.HIGHEST, preferred_element_type=jnp.float32
        )
        minus = jnp.logical_and(row < 40, iota((PACK, 128), 1) < 64)
        merid_out[0] = jnp.where(minus, -mirrored, mirrored)

    @pl.when(bottom)
    def _():
        for k in range(3):
            merid_in[3 + k] = jnp.zeros((PACK, 128), jnp.float32)

    expected = ny + nz + ngy - 3 + 2 + 1 + jnp.where(bottom, 0, 3)
    for k in (1, 2):
        expected = expected + jnp.where(mirror_self[k - 1], 0, 1)
    pl.semaphore_wait(barrier, expected)

    def remote(src, dst, sent, got, device):
        return pltpu.make_async_remote_copy(
            src_ref=src,
            dst_ref=dst,
            send_sem=halo_send.at[sent],
            recv_sem=halo_recv.at[got],
            device_id=device,
            device_id_type=MESH,
        )

    slot_of = (0, 2, 1)
    fold = [remote(merid_out.at[0], merid_in.at[k], k, k, norths[k]) for k in range(3)]
    up = [
        remote(merid_out.at[0], merid_in.at[3 + slot_of[k]], k, 3 + slot_of[k], norths[k])
        for k in range(3)
    ]
    down = [
        remote(merid_out.at[1], merid_in.at[slot_of[k]], 3 + k, slot_of[k], souths[k]) for k in range(3)
    ]
    to_east = remote(zonal_out.at[0], zonal_in.at[0], 6, 6, east)
    to_west = remote(zonal_out.at[1], zonal_in.at[1], 7, 7, west)

    @pl.when(top)
    def _():
        fold[0].start()

    for k in (1, 2):

        @pl.when(jnp.logical_and(top, jnp.logical_not(mirror_self[k - 1])))
        def _():
            fold[k].start()

        @pl.when(mirror_self[k - 1])
        def _():
            merid_in[k] = merid_out[0]

    @pl.when(jnp.logical_not(top))
    def _():
        for copy in up:
            copy.start()

    @pl.when(jnp.logical_not(bottom))
    def _():
        for copy in down:
            copy.start()

    to_east.start()
    to_west.start()

    to_east.wait_recv()
    to_west.wait_recv()

    for t in range(5):
        from_west = zonal_in[0, t]
        from_east = zonal_in[1, t]
        fields[2 * t, ROWS:EXT_ROWS, 0:COLS] = jnp.where(sub < 4, from_east, from_west)
        if t < 4:
            fields[2 * t + 1, ROWS:EXT_ROWS, 0:COLS] = jnp.where(
                sub < 4, pltpu.roll(from_east, 3, 0), pltpu.roll(from_west, 5, 0)
            )

    def arrived(k):
        remote(merid_out.at[0], merid_in.at[k], k, k, east).wait_recv()

    arrived(0)
    for k in (1, 2):

        @pl.when(jnp.logical_not(mirror_self[k - 1]))
        def _():
            arrived(k)

    @pl.when(jnp.logical_not(bottom))
    def _():
        for k in range(3):
            arrived(3 + k)

    north_side = lax.rem(iota((PACK, 128), 0), 8) < 4
    plane, from_e, from_w = [jnp.where(north_side, merid_in[k], merid_in[3 + k]) for k in range(3)]
    lane = iota((PACK, 128), 1)
    pad = jnp.zeros((128 - PACK, 128), jnp.float32)
    for g, group in enumerate(GROUPS):
        if g == 0:
            center, right, left = plane, pltpu.roll(from_e, 64, 1), pltpu.roll(from_w, 8, 1)
        else:
            center, right, left = pltpu.roll(plane, 64, 1), from_e, pltpu.roll(from_w, 72, 1)
        merged = jnp.where(lane < 64, center, jnp.where(lane < 68, right, left))
        back = jnp.transpose(jnp.concatenate([merged, pad], axis=0))[0:EXT_ROWS]
        for k, f in enumerate(group):
            fields[f, :, COLS:EXT_COLS] = pltpu.roll(back, 128 - 8 * (k + 1), 1)

    b_i = fields[B_I]
    b_o = fields[B_O]
    turn = fields[TURN]
    t_in = inner_block(turn)
    h_u, h_v, h_o = local[0], local[1], local[2]
    r_i, r_o, p_i, p_o = local[3], local[4], local[5], local[6]
    nb_u = around(fields[M_U])
    nb_v = around(fields[M_V])
    nb_o = around(fields[M_O])
    s0_u = fields[H_U] + b_i * nb_u
    s0_v = fields[H_V] + b_i * nb_v
    s0_o = fields[H_O] + b_o * nb_o
    res_u = h_u + r_i * inner_block(nb_u)
    res_v = h_v + r_i * inner_block(nb_v)
    res_o = h_o + r_o * inner_block(nb_o)
    nb_u = around(s0_u)
    nb_v = around(s0_v)
    nb_o = around(s0_o)
    s1_u = b_i * nb_u + turn * s0_v
    s1_v = b_i * nb_v - turn * s0_u
    s1_o = b_o * nb_o
    n1_u = r_i * inner_block(nb_u) + t_in * res_v
    n1_v = r_i * inner_block(nb_v) - t_in * res_u
    n1_o = r_o * inner_block(nb_o)
    n2_u = r_i * inner_block(around(s1_u)) + t_in * n1_v
    n2_v = r_i * inner_block(around(s1_v)) - t_in * n1_u
    n2_o = r_o * inner_block(around(s1_o))
    a_u, a_v, a_o = res_u - n1_u, res_v - n1_v, res_o - n1_o
    e_u, e_v, e_o = n1_u - n2_u, n1_v - n2_v, n1_o - n2_o
    z_o = p_o * res_o
    x_o = p_o * n1_o
    products = [
        a_u * a_u + a_v * a_v,
        a_u * e_u + a_v * e_v,
        e_u * e_u + e_v * e_v,
        a_u * res_u + a_v * res_v,
        e_u * res_u + e_v * res_v,
        z_o * a_o,
        x_o * a_o,
        x_o * e_o,
        z_o * res_o,
        x_o * res_o,
    ]
    local[0] = p_i * res_u
    local[1] = p_i * res_v
    local[2] = z_o
    local[3] = p_i * n1_u
    local[4] = p_i * n1_v
    local[5] = x_o

    row = iota((16, 128), 0)
    sums = jnp.zeros((16, 128), jnp.float32)
    for k, product in enumerate(products):
        half = product[:, 0:128] + product[:, 128:256]
        sums = jnp.where(row == k, jnp.sum(half, axis=0, keepdims=True), sums)
    sums = jnp.sum(sums, axis=1, keepdims=True)
    mine = jnp.sum(jnp.where(row == iota((16, 128), 1), sums, 0.0), axis=0, keepdims=True)

    def gather(value, slots, send, recv, me, peers, device_of):
        count = len(peers) + 1
        slots[me] = value
        copies = []
        for d, p in enumerate(peers):
            copy = pltpu.make_async_remote_copy(
                src_ref=slots.at[me],
                dst_ref=slots.at[me],
                send_sem=send.at[d],
                recv_sem=recv.at[me],
                device_id=device_of(p),
                device_id_type=MESH,
            )
            copy.start()
            copies.append(copy)
        for d, p in enumerate(peers):
            pltpu.make_async_remote_copy(
                src_ref=slots.at[p],
                dst_ref=slots.at[p],
                send_sem=send.at[d],
                recv_sem=recv.at[p],
                device_id=device_of(p),
                device_id_type=MESH,
            ).wait_recv()
        total = slots[0]
        for k in range(1, count):
            total = total + slots[k]
        return total, copies

    total, sent_gy = gather(mine, sum_gy, gy_send, gy_recv, gy, gy_peers, lambda p: (gx, p))
    total, sent_z = gather(total, sum_z, z_send, z_recv, zz, z_peers, lambda p: (yy * nz + p, gy))
    total, sent_y = gather(total, sum_y, y_send, y_recv, yy, y_peers, lambda p: (p * nz + zz, gy))

    def item(k):
        return total[0:1, k : k + 1]

    def solve(k11, k12, k22, k1, k2):
        scale = 1.0 / item(k11)
        a12, a22 = item(k12) * scale, item(k22) * scale
        f1, f2 = item(k1) * scale, item(k2) * scale
        det = 1.0 / (a22 - a12 * a12)
        return (a22 * f1 - a12 * f2) * det, (f2 - a12 * f1) * det

    c1, c2 = solve(0, 1, 2, 3, 4)
    d1, d2 = solve(5, 6, 7, 8, 9)
    velocity[0] = v_guess[0] + c1 * local[0] + c2 * local[3]
    velocity[1] = v_guess[1] + c1 * local[1] + c2 * local[4]
    level[...] = v_oguess[...] + d1 * local[2] + d2 * local[5]

    @pl.when(top)
    def _():
        fold[0].wait_send()

    for k in (1, 2):

        @pl.when(jnp.logical_and(top, jnp.logical_not(mirror_self[k - 1])))
        def _():
            fold[k].wait_send()

    @pl.when(jnp.logical_not(top))
    def _():
        for copy in up:
            copy.wait_send()

    @pl.when(jnp.logical_not(bottom))
    def _():
        for k in range(3):
            down[k].wait_send()

    to_east.wait_send()
    to_west.wait_send()
    for copy in sent_gy + sent_z + sent_y:
        copy.wait_send()


def build(mesh, ny, nz, interpret=False):
    ngy = mesh.shape["gy"]
    f32 = jnp.float32
    block = pltpu.VMEM((ROWS, COLS), f32)
    pair = pltpu.VMEM((2, ROWS, COLS), f32)
    whole = pltpu.VMEM((ROWS, COLS), jnp.int32)
    dma = pltpu.SemaphoreType.DMA

    def body(*args):
        return pl.pallas_call(
            functools.partial(kernel, (ny, nz, ngy)),
            out_shape=(
                jax.ShapeDtypeStruct((2, ROWS, COLS), f32),
                jax.ShapeDtypeStruct((ROWS, COLS), f32),
            ),
            in_specs=[pl.BlockSpec(memory_space=pl.ANY)] * 10,
            out_specs=(pl.BlockSpec(memory_space=pltpu.VMEM), pl.BlockSpec(memory_space=pltpu.VMEM)),
            scratch_shapes=[
                pair,
                pair,
                block,
                block,
                block,
                block,
                block,
                block,
                whole,
                whole,
                pltpu.VMEM((9, EXT_ROWS, EXT_COLS), f32),
                pltpu.VMEM((7, ROWS, COLS), f32),
                pltpu.VMEM((2, 5, 8, COLS), f32),
                pltpu.VMEM((2, 5, 8, COLS), f32),
                pltpu.VMEM((2, PACK, 128), f32),
                pltpu.VMEM((6, PACK, 128), f32),
                pltpu.VMEM((ngy, 1, 128), f32),
                pltpu.VMEM((nz, 1, 128), f32),
                pltpu.VMEM((ny, 1, 128), f32),
                dma((10,)),
                dma((8,)),
                dma((8,)),
                dma((ngy - 1,)),
                dma((ngy,)),
                dma((nz - 1,)),
                dma((nz,)),
                dma((ny - 1,)),
                dma((ny,)),
            ],
            compiler_params=pltpu.CompilerParams(collective_id=0, has_side_effects=True),
            name="picard",
        )(*args)

    both = P(None, "gx", "gy")
    one = P("gx", "gy")
    return jax.shard_map(
        body,
        mesh=mesh,
        in_specs=(both, both, one, one, one, one, one, one, one, one),
        out_specs=(both, one),
        check_vma=False,
    )


def solution(mesh):
    return build(mesh, 8, 12)
```

```python
import functools

import jax
import jax.numpy as jnp
from jax import lax
from jax.experimental import pallas as pl
from jax.experimental.pallas import tpu as pltpu
from jax.sharding import PartitionSpec as P

MESH = pl.DeviceIdType.MESH

M_U, M_V, H_U, H_V, M_O, H_O, B_I, B_O, TURN = range(9)
DEPTH = {M_U: 3, M_V: 3, M_O: 3, H_U: 2, H_V: 2, H_O: 2, B_I: 2, B_O: 2, TURN: 1}
HALVES = ((M_U, M_V, H_U, H_V), (M_O, H_O, B_I, B_O, TURN))
TILES = ((M_U, M_V, H_U), (M_O, H_V, H_O, TURN), (B_I, B_O))
PACK = 24
HUBS = 4
ROWS = 64
COLS = 256
EXT_ROWS = ROWS + 8
EXT_COLS = COLS + 128


def iota(shape, dim):
    return lax.broadcasted_iota(jnp.int32, shape, dim)


def roll(x, by, dim):
    size = x.shape[dim]
    return x if by % size == 0 else pltpu.roll(x, by % size, dim)


def columns():
    for half, fields in enumerate(HALVES):
        at = 0
        for f in fields:
            yield half, f, at, DEPTH[f]
            at += 2 * DEPTH[f]


def packed_rows():
    for t, fields in enumerate(TILES):
        at = 0
        for f in fields:
            yield t, f, at, DEPTH[f]
            at += DEPTH[f]


def northern_rows():
    row, lane = iota((PACK, 128), 0), iota((PACK, 128), 1)
    step = jnp.full((PACK, 128), -1, jnp.int32)
    for half, _, at, n in columns():
        here = (lane < 64) if half == 0 else (lane >= 64)
        for k in range(n):
            step = jnp.where(jnp.logical_and(here, row == at + n + k), k, step)
    return step


def corners(turned):
    lane = lax.rem(iota((8, 128), 1) + 2, 64)
    first, second, third = [roll(turned[8 * t : 8 * t + 8], 4 * t, 1) for t in range(3)]
    return jnp.where(lane < 4, first, jnp.where(lane < 8, second, third))


def from_corners(tile):
    return jnp.concatenate([roll(tile, -4 * t, 1) for t in range(3)], axis=0)


def around(q):
    rows, cols = q.shape
    return (
        pltpu.roll(q, 1, 0) + pltpu.roll(q, rows - 1, 0) + pltpu.roll(q, 1, 1) + pltpu.roll(q, cols - 1, 1)
    )


def inner_block(x):
    return x[:ROWS, :COLS]


def kernel(
    sizes,
    ice_rhs,
    ice_guess,
    ocean_rhs,
    ocean_guess,
    ice_diag,
    ice_visc,
    coriolis,
    depth_factor,
    wet_mask,
    ice_mask,
    velocity,
    level,
    v_rhs,
    v_guess,
    v_orhs,
    v_oguess,
    v_diag,
    v_visc,
    v_cor,
    v_depth,
    v_wet,
    v_ice,
    fields,
    local,
    zonal_out,
    zonal_in,
    merid_out,
    merid_in,
    corner_out,
    corner_in,
    sum_gy,
    sum_plane,
    result,
    load_sems,
    halo_send,
    halo_recv,
    sum_sems,
):
    ny, nz, ngy = sizes
    ngx = ny * nz
    gx = lax.axis_index("gx")
    gy = lax.axis_index("gy")
    yy = gx // nz
    zz = lax.rem(gx, nz)
    top = gy == ngy - 1
    bottom = gy == 0

    loads = []
    for i, (src, dst) in enumerate(
        (
            (ice_rhs, v_rhs),
            (ice_guess, v_guess),
            (ocean_rhs, v_orhs),
            (ocean_guess, v_oguess),
            (ice_diag, v_diag),
            (ice_visc, v_visc),
            (coriolis, v_cor),
            (depth_factor, v_depth),
            (wet_mask, v_wet),
            (ice_mask, v_ice),
        )
    ):
        loads.append(pltpu.make_async_copy(src, dst, load_sems.at[i]))

    def wrap(x):
        return lax.rem(x + ngx, ngx)

    def north_of(step):
        there = wrap(gx + step)
        return jnp.where(top, ngx - 1 - there, there), jnp.where(top, gy, gy + 1)

    def south_of(step):
        return wrap(gx + step), jnp.where(bottom, gy, gy - 1)

    east = (wrap(gx + 1), gy)
    west = (wrap(gx - 1), gy)
    norths = [north_of(step) for step in (0, 1, -1)]
    souths = [south_of(step) for step in (0, 1, -1)]
    gy_peers = [lax.rem(gy + d, ngy) for d in range(1, ngy)]
    nhub = min(HUBS, nz - 1)
    hubs = [y * nz + z for z in range(nhub) for y in range(ny)]
    is_hub = zz < nhub
    later = [z for z in range(nhub, nz)]
    relay_of = {z: nhub - 1 if 2 * (z - nhub) < nz - nhub else 0 for z in later}

    barrier = pltpu.get_barrier_semaphore()

    def greet(device):
        pl.semaphore_signal(barrier, inc=1, device_id=device, device_id_type=MESH)

    mirror_self = [jnp.logical_and(top, norths[k][0] == gx) for k in (1, 2)]

    for copy in loads:
        copy.start()

    greet(norths[0])
    for k in (1, 2):

        @pl.when(jnp.logical_not(mirror_self[k - 1]))
        def _():
            greet(norths[k])

    greet(east)
    greet(west)
    for p in gy_peers:
        greet((gx, p))

    @pl.when(jnp.logical_not(bottom))
    def _():
        for device in souths:
            greet(device)

    @pl.when(is_hub)
    def _():
        for d in range(1, ngx):
            greet((lax.rem(gx + d, ngx), gy))

    for copy in loads:
        copy.wait()

    wet = v_wet[...].astype(jnp.float32)
    active = wet * v_ice[...].astype(jnp.float32)
    visc = v_visc[...]
    depth = v_depth[...]
    d_i = active * (v_diag[...] + 4.0 * visc * visc) + 1.0 - active
    d_o = wet * (1.0 + 4.0 * depth * depth) + 1.0 - wet
    p_i = 1.0 / d_i
    p_o = 1.0 / d_o
    r_i = active * visc
    r_o = wet * depth
    s_i = r_i * p_i
    s_o = r_o * p_o
    c = active * v_cor[...]
    g_u = v_guess[0]
    g_v = v_guess[1]
    g_o = v_oguess[...]
    h_u = v_rhs[0] - d_i * g_u + c * g_v
    h_v = v_rhs[1] - d_i * g_v - c * g_u
    h_o = v_orhs[...] - d_o * g_o
    own = {
        M_U: r_i * g_u,
        M_V: r_i * g_v,
        M_O: r_o * g_o,
        H_U: s_i * h_u,
        H_V: s_i * h_v,
        H_O: s_o * h_o,
        B_I: r_i * s_i,
        B_O: r_o * s_o,
        TURN: c * p_i,
    }
    for k, value in enumerate((h_u, h_v, h_o, r_i, r_o, p_i, p_o)):
        local[k] = value
    for f in range(9):
        fields[f, 0:ROWS, 0:COLS] = own[f]

    sub = iota((8, COLS), 0)
    eastward = [jnp.zeros((8, COLS), jnp.float32)] * len(TILES)
    westward = [jnp.zeros((8, COLS), jnp.float32)] * len(TILES)
    for t, f, at, n in packed_rows():
        eastward[t] = jnp.where(
            jnp.logical_and(sub >= 8 - at - n, sub < 8 - at), roll(own[f][ROWS - 8 : ROWS], -at, 0), eastward[t]
        )
        westward[t] = jnp.where(jnp.logical_and(sub >= at, sub < at + n), roll(own[f][0:8], at, 0), westward[t])
    for t in range(len(TILES)):
        zonal_out[0, t] = eastward[t]
        zonal_out[1, t] = westward[t]

    lane = iota((ROWS, 128), 1)
    halves = [jnp.zeros((ROWS, 128), jnp.float32)] * 2
    for half, f, at, n in columns():
        edge = jnp.where(lane < 64, own[f][:, 0:128], own[f][:, COLS - 128 : COLS])
        halves[half] = jnp.where(
            jnp.logical_and(lane >= at, lane < at + 2 * n), roll(edge, at + n, 1), halves[half]
        )
    turned = jnp.transpose(jnp.concatenate(halves, axis=0))[0:PACK]
    merid_out[0] = turned
    merid_out[1] = turned
    corner_out[0] = corners(turned)
    corner_out[1] = corners(turned)

    @pl.when(top)
    def _():
        step = northern_rows()
        flipped = jnp.where(
            step == 0, roll(turned, 1, 0), jnp.where(step == 1, roll(turned, 3, 0), roll(turned, 5, 0))
        )
        swap = jnp.where(
            (iota((128, 128), 0) ^ iota((128, 128), 1)) == 63, 1.0, 0.0
        ).astype(jnp.float32)
        mirrored = jnp.dot(
            flipped, swap, precision=lax.Precision.HIGHEST, preferred_element_type=jnp.float32
        )
        mirrored = jnp.where(iota((PACK, 128), 1) < 64, -mirrored, mirrored)
        merid_out[0] = mirrored
        corner_out[0] = corners(mirrored)

    @pl.when(bottom)
    def _():
        merid_in[1] = jnp.zeros((PACK, 128), jnp.float32)
        for k in (2, 3):
            corner_in[k] = jnp.zeros((8, 128), jnp.float32)

    expected = len(hubs) + ngy - 1 + 2 + 1 + jnp.where(bottom, 0, 3) - jnp.where(is_hub, 1, 0)
    for k in (1, 2):
        expected = expected + jnp.where(mirror_self[k - 1], 0, 1)
    pl.semaphore_wait(barrier, expected)

    def remote(src, dst, sent, got, device):
        return pltpu.make_async_remote_copy(
            src_ref=src,
            dst_ref=dst,
            send_sem=halo_send.at[sent],
            recv_sem=halo_recv.at[got],
            device_id=device,
            device_id_type=MESH,
        )

    fold = [
        remote(merid_out.at[0], merid_in.at[0], 0, 0, norths[0]),
        remote(corner_out.at[0], corner_in.at[0], 1, 2, norths[1]),
        remote(corner_out.at[0], corner_in.at[1], 2, 3, norths[2]),
    ]
    up = [
        remote(merid_out.at[0], merid_in.at[1], 0, 1, norths[0]),
        remote(corner_out.at[0], corner_in.at[3], 1, 5, norths[1]),
        remote(corner_out.at[0], corner_in.at[2], 2, 4, norths[2]),
    ]
    down = [
        remote(merid_out.at[1], merid_in.at[0], 3, 0, souths[0]),
        remote(corner_out.at[1], corner_in.at[1], 4, 3, souths[1]),
        remote(corner_out.at[1], corner_in.at[0], 5, 2, souths[2]),
    ]
    to_east = remote(zonal_out.at[0], zonal_in.at[0], 6, 6, east)
    to_west = remote(zonal_out.at[1], zonal_in.at[1], 7, 7, west)

    @pl.when(top)
    def _():
        fold[0].start()

    for k in (1, 2):

        @pl.when(jnp.logical_and(top, jnp.logical_not(mirror_self[k - 1])))
        def _():
            fold[k].start()

        @pl.when(mirror_self[k - 1])
        def _():
            corner_in[k - 1] = corner_out[0]

    @pl.when(jnp.logical_not(top))
    def _():
        for copy in up:
            copy.start()

    @pl.when(jnp.logical_not(bottom))
    def _():
        for copy in down:
            copy.start()

    to_east.start()
    to_west.start()

    to_east.wait_recv()
    to_west.wait_recv()

    for t, f, at, n in packed_rows():
        fields[f, ROWS:EXT_ROWS, 0:COLS] = jnp.where(
            sub < 4, roll(zonal_in[1, t], -at, 0), roll(zonal_in[0, t], at, 0)
        )

    def arrived(k, src, dst):
        remote(src, dst, k, k, east).wait_recv()

    arrived(0, merid_out.at[0], merid_in.at[0])
    for k in (1, 2):

        @pl.when(jnp.logical_not(mirror_self[k - 1]))
        def _():
            arrived(1 + k, corner_out.at[0], corner_in.at[k - 1])

    @pl.when(jnp.logical_not(bottom))
    def _():
        arrived(1, merid_out.at[0], merid_in.at[1])
        for k in (2, 3):
            arrived(2 + k, corner_out.at[0], corner_in.at[k])

    northern = northern_rows() >= 0
    plane = jnp.where(northern, merid_in[0], merid_in[1])
    from_e = jnp.where(northern, from_corners(corner_in[0]), from_corners(corner_in[2]))
    from_w = jnp.where(northern, from_corners(corner_in[1]), from_corners(corner_in[3]))
    lane = iota((PACK, 128), 1)
    pad = jnp.zeros((128 - PACK, 128), jnp.float32)
    backs = []
    for half in range(2):
        if half == 0:
            center, right, left = plane, roll(from_e, 64, 1), roll(from_w, 8, 1)
        else:
            center, right, left = roll(plane, 64, 1), from_e, roll(from_w, 72, 1)
        merged = jnp.where(lane < 64, center, jnp.where(lane < 68, right, left))
        backs.append(jnp.transpose(jnp.concatenate([merged, pad], axis=0))[0:EXT_ROWS])
    for half, f, at, n in columns():
        fields[f, :, COLS:EXT_COLS] = roll(backs[half], -(at + n), 1)

    b_i = fields[B_I]
    b_o = fields[B_O]
    turn = fields[TURN]
    t_in = inner_block(turn)
    h_u, h_v, h_o = local[0], local[1], local[2]
    r_i, r_o, p_i, p_o = local[3], local[4], local[5], local[6]
    nb_u = around(fields[M_U])
    nb_v = around(fields[M_V])
    nb_o = around(fields[M_O])
    s0_u = fields[H_U] + b_i * nb_u
    s0_v = fields[H_V] + b_i * nb_v
    s0_o = fields[H_O] + b_o * nb_o
    res_u = h_u + r_i * inner_block(nb_u)
    res_v = h_v + r_i * inner_block(nb_v)
    res_o = h_o + r_o * inner_block(nb_o)
    nb_u = around(s0_u)
    nb_v = around(s0_v)
    nb_o = around(s0_o)
    s1_u = b_i * nb_u + turn * s0_v
    s1_v = b_i * nb_v - turn * s0_u
    s1_o = b_o * nb_o
    n1_u = r_i * inner_block(nb_u) + t_in * res_v
    n1_v = r_i * inner_block(nb_v) - t_in * res_u
    n1_o = r_o * inner_block(nb_o)
    n2_u = r_i * inner_block(around(s1_u)) + t_in * n1_v
    n2_v = r_i * inner_block(around(s1_v)) - t_in * n1_u
    n2_o = r_o * inner_block(around(s1_o))
    a_u, a_v, a_o = res_u - n1_u, res_v - n1_v, res_o - n1_o
    e_u, e_v, e_o = n1_u - n2_u, n1_v - n2_v, n1_o - n2_o
    z_o = p_o * res_o
    x_o = p_o * n1_o
    products = [
        a_u * a_u + a_v * a_v,
        a_u * e_u + a_v * e_v,
        e_u * e_u + e_v * e_v,
        a_u * res_u + a_v * res_v,
        e_u * res_u + e_v * res_v,
        z_o * a_o,
        x_o * a_o,
        x_o * e_o,
        z_o * res_o,
        x_o * res_o,
    ]
    local[0] = p_i * res_u
    local[1] = p_i * res_v
    local[2] = z_o
    local[3] = p_i * n1_u
    local[4] = p_i * n1_v
    local[5] = x_o

    row = iota((16, 128), 0)
    sums = jnp.zeros((16, 128), jnp.float32)
    for k, product in enumerate(products):
        half = product[:, 0:128] + product[:, 128:256]
        sums = jnp.where(row == k, jnp.sum(half, axis=0, keepdims=True), sums)
    sums = jnp.sum(sums, axis=1, keepdims=True)
    mine = jnp.sum(jnp.where(row == iota((16, 128), 1), sums, 0.0), axis=0, keepdims=True)

    def rows_of(slots, count, sem):
        return pltpu.make_async_copy(slots.at[pl.ds(0, count)], slots.at[pl.ds(0, count)], sem)

    def send_row(slots, at, dst, dst_at, send, recv, device):
        pltpu.make_async_remote_copy(
            src_ref=slots.at[at],
            dst_ref=dst.at[dst_at],
            send_sem=sum_sems.at[send],
            recv_sem=sum_sems.at[recv],
            device_id=device,
            device_id_type=MESH,
        ).start()

    sum_gy[gy] = mine
    for p in gy_peers:
        send_row(sum_gy, gy, sum_gy, gy, 0, 1, (gx, p))
    rows_of(sum_gy, ngy - 1, sum_sems.at[1]).wait()
    total = sum_gy[0]
    for k in range(1, ngy):
        total = total + sum_gy[k]

    sum_plane[gx] = total
    for hub in hubs:

        @pl.when(gx != hub)
        def _():
            send_row(sum_plane, gx, sum_plane, gx, 2, 3, (hub, gy))

    @pl.when(is_hub)
    def _():
        rows_of(sum_plane, ngx - 1, sum_sems.at[3]).wait()
        whole = sum_plane[0]
        for k in range(1, ngx):
            whole = whole + sum_plane[k]
        result[0] = whole
        result[1] = whole
        for z in later:

            @pl.when(zz == relay_of[z])
            def _():
                send_row(result, 0, result, 1, 4, 5, (yy * nz + z, gy))

    @pl.when(jnp.logical_not(is_hub))
    def _():
        rows_of(result, 1, sum_sems.at[5]).wait()

    total = result[1]

    def item(k):
        return total[0:1, k : k + 1]

    def solve(k11, k12, k22, k1, k2):
        scale = 1.0 / item(k11)
        a12, a22 = item(k12) * scale, item(k22) * scale
        f1, f2 = item(k1) * scale, item(k2) * scale
        det = 1.0 / (a22 - a12 * a12)
        return (a22 * f1 - a12 * f2) * det, (f2 - a12 * f1) * det

    c1, c2 = solve(0, 1, 2, 3, 4)
    d1, d2 = solve(5, 6, 7, 8, 9)
    velocity[0] = v_guess[0] + c1 * local[0] + c2 * local[3]
    velocity[1] = v_guess[1] + c1 * local[1] + c2 * local[4]
    level[...] = v_oguess[...] + d1 * local[2] + d2 * local[5]

    @pl.when(top)
    def _():
        fold[0].wait_send()

    for k in (1, 2):

        @pl.when(jnp.logical_and(top, jnp.logical_not(mirror_self[k - 1])))
        def _():
            fold[k].wait_send()

    @pl.when(jnp.logical_not(top))
    def _():
        for copy in up:
            copy.wait_send()

    @pl.when(jnp.logical_not(bottom))
    def _():
        for k in range(3):
            down[k].wait_send()

    to_east.wait_send()
    to_west.wait_send()
    rows_of(sum_gy, ngy - 1, sum_sems.at[0]).wait()

    @pl.when(is_hub)
    def _():
        rows_of(sum_plane, len(hubs) - 1, sum_sems.at[2]).wait()

    @pl.when(jnp.logical_not(is_hub))
    def _():
        rows_of(sum_plane, len(hubs), sum_sems.at[2]).wait()

    for hub in range(nhub):
        served = len([z for z in later if relay_of[z] == hub])
        if served:

            @pl.when(zz == hub)
            def _():
                rows_of(sum_plane, served, sum_sems.at[4]).wait()


def build(mesh, ny, nz, interpret=False):
    ngy = mesh.shape["gy"]
    f32 = jnp.float32
    block = pltpu.VMEM((ROWS, COLS), f32)
    pair = pltpu.VMEM((2, ROWS, COLS), f32)
    whole = pltpu.VMEM((ROWS, COLS), jnp.int32)
    dma = pltpu.SemaphoreType.DMA

    def body(*args):
        return pl.pallas_call(
            functools.partial(kernel, (ny, nz, ngy)),
            out_shape=(
                pltpu.VMEM((2, ROWS, COLS), f32),
                pltpu.VMEM((ROWS, COLS), f32),
            ),
            in_specs=[pl.BlockSpec(memory_space=pl.ANY)] * 10,
            out_specs=(pl.BlockSpec(memory_space=pltpu.VMEM), pl.BlockSpec(memory_space=pltpu.VMEM)),
            scratch_shapes=[
                pair,
                pair,
                block,
                block,
                block,
                block,
                block,
                block,
                whole,
                whole,
                pltpu.VMEM((9, EXT_ROWS, EXT_COLS), f32),
                pltpu.VMEM((7, ROWS, COLS), f32),
                pltpu.VMEM((2, 3, 8, COLS), f32),
                pltpu.VMEM((2, 3, 8, COLS), f32),
                pltpu.VMEM((2, PACK, 128), f32),
                pltpu.VMEM((2, PACK, 128), f32),
                pltpu.VMEM((2, 8, 128), f32),
                pltpu.VMEM((4, 8, 128), f32),
                pltpu.VMEM((ngy, 1, 128), f32),
                pltpu.VMEM((ny * nz, 1, 128), f32),
                pltpu.VMEM((2, 1, 128), f32),
                dma((10,)),
                dma((8,)),
                dma((8,)),
                dma((6,)),
            ],
            compiler_params=pltpu.CompilerParams(collective_id=0, has_side_effects=True, vmem_limit_bytes=16 * 1024 * 1024),
            name="picard",
        )(*[pltpu.with_memory_space_constraint(a, pltpu.HBM) for a in args])

    both = P(None, "gx", "gy")
    one = P("gx", "gy")
    return jax.shard_map(
        body,
        mesh=mesh,
        in_specs=(both, both, one, one, one, one, one, one, one, one),
        out_specs=(both, one),
        check_vma=False,
    )


def solution(mesh):
    return build(mesh, 8, 12)
```

```python
import functools

import jax
import jax.numpy as jnp
from jax import lax
from jax.experimental import pallas as pl
from jax.experimental.pallas import tpu as pltpu
from jax.sharding import PartitionSpec as P

MESH = pl.DeviceIdType.MESH

M_U, M_V, H_U, H_V, M_O, H_O, B_I, B_O, TURN = range(9)
DEPTH = {M_U: 3, M_V: 3, M_O: 3, H_U: 2, H_V: 2, H_O: 2, B_I: 2, B_O: 2, TURN: 1}
HALVES = ((M_U, M_V, H_U, H_V), (M_O, H_O, B_I, B_O, TURN))
TILES = ((M_U, M_V, H_U), (M_O, H_V, H_O, TURN), (B_I, B_O))
PACK = 24
STRIP = PACK + 16
HUBS = 4
ROWS = 64
COLS = 256
EXT_ROWS = ROWS + 8
EXT_COLS = COLS + 128


def iota(shape, dim):
    return lax.broadcasted_iota(jnp.int32, shape, dim)


def roll(x, by, dim):
    size = x.shape[dim]
    return x if by % size == 0 else pltpu.roll(x, by % size, dim)


def columns():
    for half, fields in enumerate(HALVES):
        at = 0
        for f in fields:
            yield half, f, at, DEPTH[f]
            at += 2 * DEPTH[f]


def packed_rows():
    for t, fields in enumerate(TILES):
        at = 0
        for f in fields:
            yield t, f, at, DEPTH[f]
            at += DEPTH[f]


def northern_rows():
    row, lane = iota((PACK, 128), 0), iota((PACK, 128), 1)
    step = jnp.full((PACK, 128), -1, jnp.int32)
    for half, _, at, n in columns():
        here = (lane < 64) if half == 0 else (lane >= 64)
        for k in range(n):
            step = jnp.where(jnp.logical_and(here, row == at + n + k), k, step)
    return step


def corners(turned):
    lane = lax.rem(iota((8, 128), 1) + 2, 64)
    first, second, third = [roll(turned[8 * t : 8 * t + 8], 4 * t, 1) for t in range(3)]
    return jnp.where(lane < 4, first, jnp.where(lane < 8, second, third))


def from_corners(tile):
    return jnp.concatenate([roll(tile, -4 * t, 1) for t in range(3)], axis=0)


def around(q):
    rows, cols = q.shape
    return (
        pltpu.roll(q, 1, 0) + pltpu.roll(q, rows - 1, 0) + pltpu.roll(q, 1, 1) + pltpu.roll(q, cols - 1, 1)
    )


def inner_block(x):
    return x[:ROWS, :COLS]


def kernel(
    sizes,
    ice_rhs,
    ice_guess,
    ocean_rhs,
    ocean_guess,
    ice_diag,
    ice_visc,
    coriolis,
    depth_factor,
    wet_mask,
    ice_mask,
    velocity,
    level,
    v_rhs,
    v_guess,
    v_orhs,
    v_oguess,
    v_diag,
    v_visc,
    v_cor,
    v_depth,
    v_wet,
    v_ice,
    fields,
    local,
    zonal_out,
    zonal_in,
    merid_out,
    corner_out,
    north_in,
    south_in,
    post_in,
    sum_gy,
    sum_plane,
    result,
    load_sems,
    halo_send,
    halo_recv,
    post_send,
    post_recv,
    sum_sems,
):
    ny, nz, ngy = sizes
    ngx = ny * nz
    gx = lax.axis_index("gx")
    gy = lax.axis_index("gy")
    yy = gx // nz
    zz = lax.rem(gx, nz)
    top = gy == ngy - 1
    bottom = gy == 0

    loads = []
    for i, (src, dst) in enumerate(
        (
            (ice_rhs, v_rhs),
            (ice_guess, v_guess),
            (ocean_rhs, v_orhs),
            (ocean_guess, v_oguess),
            (ice_diag, v_diag),
            (ice_visc, v_visc),
            (coriolis, v_cor),
            (depth_factor, v_depth),
            (wet_mask, v_wet),
            (ice_mask, v_ice),
        )
    ):
        loads.append(pltpu.make_async_copy(src, dst, load_sems.at[i]))

    def wrap(x):
        return lax.rem(x + ngx, ngx)

    def north_of(step):
        there = wrap(gx + step)
        return jnp.where(top, ngx - 1 - there, there), jnp.where(top, gy, gy + 1)

    def south_of(step):
        return wrap(gx + step), jnp.where(bottom, gy, gy - 1)

    east = (wrap(gx + 1), gy)
    west = (wrap(gx - 1), gy)
    norths = [north_of(step) for step in (0, 1, -1)]
    souths = [south_of(step) for step in (0, 1, -1)]
    gy_peers = [lax.rem(gy + d, ngy) for d in range(1, ngy)]
    nhub = min(HUBS, nz - 1)
    hubs = [y * nz + z for z in range(nhub) for y in range(ny)]
    is_hub = zz < nhub
    later = [z for z in range(nhub, nz)]

    barrier = pltpu.get_barrier_semaphore()

    def greet(device):
        pl.semaphore_signal(barrier, inc=1, device_id=device, device_id_type=MESH)

    far_z = 2 * nz // 3
    posts = {}
    for z in range(nz // 2, nz):
        posts.setdefault(0 if z >= far_z else nz - 1 - z, []).append(z)

    def is_late(g):
        return 2 * lax.rem(g, nz) >= nz

    def post_of(g):
        z = lax.rem(g, nz)
        far = z >= far_z
        return g - z + jnp.where(far, 0, nz - 1 - z), jnp.where(far, z - far_z, 0)

    def mirrors(g):
        return [ngx - 1 - wrap(g + step) for step in (0, 1, -1)]

    late = is_late(gx)
    mirror_self = [
        jnp.logical_and(jnp.logical_and(top, jnp.logical_not(late)), norths[k][0] == gx) for k in range(3)
    ]

    for copy in loads:
        copy.start()

    @pl.when(jnp.logical_and(top, late))
    def _():
        greet((post_of(gx)[0], gy))

    for k in range(3):

        @pl.when(jnp.logical_not(jnp.logical_or(jnp.logical_and(top, late), mirror_self[k])))
        def _():
            greet(norths[k])

    greet(east)
    greet(west)
    for p in gy_peers:
        greet((gx, p))

    @pl.when(jnp.logical_not(bottom))
    def _():
        for device in souths:
            greet(device)

    for at, served in posts.items():

        @pl.when(jnp.logical_and(top, zz == at))
        def _():
            for z in served:
                for g in mirrors(yy * nz + z):
                    greet((g, gy))

    @pl.when(is_hub)
    def _():
        for d in range(1, ngx):
            greet((lax.rem(gx + d, ngx), gy))

    for copy in loads:
        copy.wait()

    wet = v_wet[...].astype(jnp.float32)
    active = wet * v_ice[...].astype(jnp.float32)
    visc = v_visc[...]
    depth = v_depth[...]
    d_i = active * (v_diag[...] + 4.0 * visc * visc) + 1.0 - active
    d_o = wet * (1.0 + 4.0 * depth * depth) + 1.0 - wet
    p_i = 1.0 / d_i
    p_o = 1.0 / d_o
    r_i = active * visc
    r_o = wet * depth
    s_i = r_i * p_i
    s_o = r_o * p_o
    c = active * v_cor[...]
    g_u = v_guess[0]
    g_v = v_guess[1]
    g_o = v_oguess[...]
    h_u = v_rhs[0] - d_i * g_u + c * g_v
    h_v = v_rhs[1] - d_i * g_v - c * g_u
    h_o = v_orhs[...] - d_o * g_o
    own = {
        M_U: r_i * g_u,
        M_V: r_i * g_v,
        M_O: r_o * g_o,
        H_U: s_i * h_u,
        H_V: s_i * h_v,
        H_O: s_o * h_o,
        B_I: r_i * s_i,
        B_O: r_o * s_o,
        TURN: c * p_i,
    }
    for k, value in enumerate((h_u, h_v, h_o, r_i, r_o, p_i, p_o)):
        local[k] = value
    for f in range(9):
        fields[f, 0:ROWS, 0:COLS] = own[f]

    sub = iota((8, COLS), 0)
    eastward = [jnp.zeros((8, COLS), jnp.float32)] * len(TILES)
    westward = [jnp.zeros((8, COLS), jnp.float32)] * len(TILES)
    for t, f, at, n in packed_rows():
        eastward[t] = jnp.where(
            jnp.logical_and(sub >= 8 - at - n, sub < 8 - at), roll(own[f][ROWS - 8 : ROWS], -at, 0), eastward[t]
        )
        westward[t] = jnp.where(jnp.logical_and(sub >= at, sub < at + n), roll(own[f][0:8], at, 0), westward[t])
    for t in range(len(TILES)):
        zonal_out[0, t] = eastward[t]
        zonal_out[1, t] = westward[t]

    lane = iota((ROWS, 128), 1)
    halves = [jnp.zeros((ROWS, 128), jnp.float32)] * 2
    for half, f, at, n in columns():
        edge = jnp.where(lane < 64, own[f][:, 0:128], own[f][:, COLS - 128 : COLS])
        halves[half] = jnp.where(
            jnp.logical_and(lane >= at, lane < at + 2 * n), roll(edge, at + n, 1), halves[half]
        )
    turned = jnp.transpose(jnp.concatenate(halves, axis=0))[0:PACK]
    merid_out[0] = turned
    merid_out[1] = turned
    corner_out[0] = corners(turned)
    corner_out[1] = corners(turned)

    @pl.when(top)
    def _():
        step = northern_rows()
        flipped = jnp.where(
            step == 0, roll(turned, 1, 0), jnp.where(step == 1, roll(turned, 3, 0), roll(turned, 5, 0))
        )
        swap = jnp.where(
            (iota((128, 128), 0) ^ iota((128, 128), 1)) == 63, 1.0, 0.0
        ).astype(jnp.float32)
        mirrored = jnp.dot(
            flipped, swap, precision=lax.Precision.HIGHEST, preferred_element_type=jnp.float32
        )
        mirrored = jnp.where(iota((PACK, 128), 1) < 64, -mirrored, mirrored)
        merid_out[0] = mirrored
        corner_out[0] = corners(mirrored)

    @pl.when(bottom)
    def _():
        south_in[...] = jnp.zeros((STRIP, 128), jnp.float32)

    expected = len(hubs) + ngy - 1 + 2 + 3 + jnp.where(bottom, 0, 3) - jnp.where(is_hub, 1, 0)
    for k in range(3):
        expected = expected - jnp.where(mirror_self[k], 1, 0)
    for at, served in posts.items():
        expected = expected + jnp.where(jnp.logical_and(top, zz == at), len(served), 0)
    pl.semaphore_wait(barrier, expected)

    def remote(src, dst, sent, got, device):
        return pltpu.make_async_remote_copy(
            src_ref=src,
            dst_ref=dst,
            send_sem=halo_send.at[sent],
            recv_sem=halo_recv.at[got],
            device_id=device,
            device_id_type=MESH,
        )

    parts = [pl.ds(0, PACK), pl.ds(PACK, 8), pl.ds(PACK + 8, 8)]
    opposite = (0, 2, 1)
    sources = [[merid_out.at[i], corner_out.at[i], corner_out.at[i]] for i in range(2)]
    fold = [remote(sources[0][k], north_in.at[parts[k]], k, k, norths[k]) for k in range(3)]
    up = [
        remote(sources[0][k], south_in.at[parts[opposite[k]]], k, 3 + opposite[k], norths[k])
        for k in range(3)
    ]
    down = [
        remote(sources[1][k], north_in.at[parts[opposite[k]]], 3 + k, opposite[k], souths[k])
        for k in range(3)
    ]

    def to_post(k):
        post, slot = post_of(norths[k][0])
        return pltpu.make_async_remote_copy(
            src_ref=sources[0][k],
            dst_ref=post_in.at[slot, parts[k]],
            send_sem=halo_send.at[k],
            recv_sem=post_recv.at[slot],
            device_id=(post, gy),
            device_id_type=MESH,
        )

    to_east = remote(zonal_out.at[0], zonal_in.at[0], 6, 6, east)
    to_west = remote(zonal_out.at[1], zonal_in.at[1], 7, 7, west)

    target_late = [is_late(norths[k][0]) for k in range(3)]
    for k in range(3):

        @pl.when(jnp.logical_and(top, target_late[k]))
        def _():
            to_post(k).start()

        @pl.when(
            jnp.logical_and(
                jnp.logical_and(top, jnp.logical_not(target_late[k])), jnp.logical_not(mirror_self[k])
            )
        )
        def _():
            fold[k].start()

        @pl.when(mirror_self[k])
        def _():
            north_in[PACK + 8 * max(k - 1, 0) : PACK + 8 * max(k - 1, 0) + 8] = corner_out[0]

    @pl.when(jnp.logical_not(top))
    def _():
        for copy in up:
            copy.start()

    @pl.when(jnp.logical_not(bottom))
    def _():
        for copy in down:
            copy.start()

    to_east.start()
    to_west.start()

    for at, served in posts.items():

        @pl.when(jnp.logical_and(top, zz == at))
        def _():
            for slot, z in enumerate(served):
                strip = post_in.at[slot]
                pltpu.make_async_copy(strip, strip, post_recv.at[slot]).wait()
                pltpu.make_async_remote_copy(
                    src_ref=strip,
                    dst_ref=north_in,
                    send_sem=post_send.at[slot],
                    recv_sem=halo_recv.at[0],
                    device_id=(yy * nz + z, gy),
                    device_id_type=MESH,
                ).start()

    to_east.wait_recv()
    to_west.wait_recv()

    for t, f, at, n in packed_rows():
        fields[f, ROWS:EXT_ROWS, 0:COLS] = jnp.where(
            sub < 4, roll(zonal_in[1, t], -at, 0), roll(zonal_in[0, t], at, 0)
        )

    def arrived(k, dst):
        pltpu.make_async_copy(dst, dst, halo_recv.at[k]).wait()

    @pl.when(jnp.logical_and(top, late))
    def _():
        arrived(0, north_in)

    for k in range(3):

        @pl.when(jnp.logical_not(jnp.logical_or(jnp.logical_and(top, late), mirror_self[k])))
        def _():
            arrived(k, north_in.at[parts[k]])

        @pl.when(jnp.logical_not(bottom))
        def _():
            arrived(3 + k, south_in.at[parts[k]])

    northern = northern_rows() >= 0
    plane = jnp.where(northern, north_in[0:PACK], south_in[0:PACK])
    from_e, from_w = [
        jnp.where(northern, from_corners(north_in[at : at + 8]), from_corners(south_in[at : at + 8]))
        for at in (PACK, PACK + 8)
    ]
    lane = iota((PACK, 128), 1)
    pad = jnp.zeros((128 - PACK, 128), jnp.float32)
    backs = []
    for half in range(2):
        if half == 0:
            center, right, left = plane, roll(from_e, 64, 1), roll(from_w, 8, 1)
        else:
            center, right, left = roll(plane, 64, 1), from_e, roll(from_w, 72, 1)
        merged = jnp.where(lane < 64, center, jnp.where(lane < 68, right, left))
        backs.append(jnp.transpose(jnp.concatenate([merged, pad], axis=0))[0:EXT_ROWS])
    for half, f, at, n in columns():
        fields[f, :, COLS:EXT_COLS] = roll(backs[half], -(at + n), 1)

    b_i = fields[B_I]
    b_o = fields[B_O]
    turn = fields[TURN]
    t_in = inner_block(turn)
    h_u, h_v, h_o = local[0], local[1], local[2]
    r_i, r_o, p_i, p_o = local[3], local[4], local[5], local[6]
    nb_u = around(fields[M_U])
    nb_v = around(fields[M_V])
    nb_o = around(fields[M_O])
    s0_u = fields[H_U] + b_i * nb_u
    s0_v = fields[H_V] + b_i * nb_v
    s0_o = fields[H_O] + b_o * nb_o
    res_u = h_u + r_i * inner_block(nb_u)
    res_v = h_v + r_i * inner_block(nb_v)
    res_o = h_o + r_o * inner_block(nb_o)
    nb_u = around(s0_u)
    nb_v = around(s0_v)
    nb_o = around(s0_o)
    s1_u = b_i * nb_u + turn * s0_v
    s1_v = b_i * nb_v - turn * s0_u
    s1_o = b_o * nb_o
    n1_u = r_i * inner_block(nb_u) + t_in * res_v
    n1_v = r_i * inner_block(nb_v) - t_in * res_u
    n1_o = r_o * inner_block(nb_o)
    n2_u = r_i * inner_block(around(s1_u)) + t_in * n1_v
    n2_v = r_i * inner_block(around(s1_v)) - t_in * n1_u
    n2_o = r_o * inner_block(around(s1_o))
    a_u, a_v, a_o = res_u - n1_u, res_v - n1_v, res_o - n1_o
    e_u, e_v, e_o = n1_u - n2_u, n1_v - n2_v, n1_o - n2_o
    z_o = p_o * res_o
    x_o = p_o * n1_o
    products = [
        a_u * a_u + a_v * a_v,
        a_u * e_u + a_v * e_v,
        e_u * e_u + e_v * e_v,
        a_u * res_u + a_v * res_v,
        e_u * res_u + e_v * res_v,
        z_o * a_o,
        x_o * a_o,
        x_o * e_o,
        z_o * res_o,
        x_o * res_o,
    ]
    local[0] = p_i * res_u
    local[1] = p_i * res_v
    local[2] = z_o
    local[3] = p_i * n1_u
    local[4] = p_i * n1_v
    local[5] = x_o

    row = iota((16, 128), 0)
    sums = jnp.zeros((16, 128), jnp.float32)
    for k, product in enumerate(products):
        half = product[:, 0:128] + product[:, 128:256]
        sums = jnp.where(row == k, jnp.sum(half, axis=0, keepdims=True), sums)
    sums = jnp.sum(sums, axis=1, keepdims=True)
    mine = jnp.sum(jnp.where(row == iota((16, 128), 1), sums, 0.0), axis=0, keepdims=True)

    def rows_of(slots, count, sem):
        return pltpu.make_async_copy(slots.at[pl.ds(0, count)], slots.at[pl.ds(0, count)], sem)

    def send_row(slots, at, dst, dst_at, send, recv, device):
        pltpu.make_async_remote_copy(
            src_ref=slots.at[at],
            dst_ref=dst.at[dst_at],
            send_sem=sum_sems.at[send],
            recv_sem=sum_sems.at[recv],
            device_id=device,
            device_id_type=MESH,
        ).start()

    sum_gy[gy] = mine
    for p in gy_peers:
        send_row(sum_gy, gy, sum_gy, gy, 0, 1, (gx, p))
    rows_of(sum_gy, ngy - 1, sum_sems.at[1]).wait()
    total = sum_gy[0]
    for k in range(1, ngy):
        total = total + sum_gy[k]

    sum_plane[gx] = total
    for hub in hubs:

        @pl.when(gx != hub)
        def _():
            send_row(sum_plane, gx, sum_plane, gx, 2, 3, (hub, gy))

    @pl.when(is_hub)
    def _():
        rows_of(sum_plane, ngx - 1, sum_sems.at[3]).wait()
        whole = sum_plane[0]
        for k in range(1, ngx):
            whole = whole + sum_plane[k]
        result[0] = whole
        result[1] = whole
        for z in later:

            @pl.when(zz == nhub - 1)
            def _():
                send_row(result, 0, result, 1, 4, 5, (yy * nz + z, gy))

    @pl.when(jnp.logical_not(is_hub))
    def _():
        rows_of(result, 1, sum_sems.at[5]).wait()

    total = result[1]

    def item(k):
        return total[0:1, k : k + 1]

    def solve(k11, k12, k22, k1, k2):
        scale = 1.0 / item(k11)
        a12, a22 = item(k12) * scale, item(k22) * scale
        f1, f2 = item(k1) * scale, item(k2) * scale
        det = 1.0 / (a22 - a12 * a12)
        return (a22 * f1 - a12 * f2) * det, (f2 - a12 * f1) * det

    c1, c2 = solve(0, 1, 2, 3, 4)
    d1, d2 = solve(5, 6, 7, 8, 9)
    velocity[0] = v_guess[0] + c1 * local[0] + c2 * local[3]
    velocity[1] = v_guess[1] + c1 * local[1] + c2 * local[4]
    level[...] = v_oguess[...] + d1 * local[2] + d2 * local[5]

    for k in range(3):

        @pl.when(jnp.logical_and(top, jnp.logical_not(mirror_self[k])))
        def _():
            fold[k].wait_send()

    for at, served in posts.items():

        @pl.when(jnp.logical_and(top, zz == at))
        def _():
            for slot, _ in enumerate(served):
                pltpu.make_async_copy(post_in.at[slot], post_in.at[slot], post_send.at[slot]).wait()

    @pl.when(jnp.logical_not(top))
    def _():
        for copy in up:
            copy.wait_send()

    @pl.when(jnp.logical_not(bottom))
    def _():
        for k in range(3):
            down[k].wait_send()

    to_east.wait_send()
    to_west.wait_send()
    rows_of(sum_gy, ngy - 1, sum_sems.at[0]).wait()

    @pl.when(is_hub)
    def _():
        rows_of(sum_plane, len(hubs) - 1, sum_sems.at[2]).wait()

    @pl.when(jnp.logical_not(is_hub))
    def _():
        rows_of(sum_plane, len(hubs), sum_sems.at[2]).wait()

    @pl.when(zz == nhub - 1)
    def _():
        rows_of(sum_plane, len(later), sum_sems.at[4]).wait()


def build(mesh, ny, nz, interpret=False):
    ngy = mesh.shape["gy"]
    f32 = jnp.float32
    block = pltpu.VMEM((ROWS, COLS), f32)
    pair = pltpu.VMEM((2, ROWS, COLS), f32)
    whole = pltpu.VMEM((ROWS, COLS), jnp.int32)
    dma = pltpu.SemaphoreType.DMA

    def body(*args):
        return pl.pallas_call(
            functools.partial(kernel, (ny, nz, ngy)),
            out_shape=(
                pltpu.VMEM((2, ROWS, COLS), f32),
                pltpu.VMEM((ROWS, COLS), f32),
            ),
            in_specs=[pl.BlockSpec(memory_space=pl.ANY)] * 10,
            out_specs=(pl.BlockSpec(memory_space=pltpu.VMEM), pl.BlockSpec(memory_space=pltpu.VMEM)),
            scratch_shapes=[
                pair,
                pair,
                block,
                block,
                block,
                block,
                block,
                block,
                whole,
                whole,
                pltpu.VMEM((9, EXT_ROWS, EXT_COLS), f32),
                pltpu.VMEM((7, ROWS, COLS), f32),
                pltpu.VMEM((2, 3, 8, COLS), f32),
                pltpu.VMEM((2, 3, 8, COLS), f32),
                pltpu.VMEM((2, PACK, 128), f32),
                pltpu.VMEM((2, 8, 128), f32),
                pltpu.VMEM((STRIP, 128), f32),
                pltpu.VMEM((STRIP, 128), f32),
                pltpu.VMEM((nz - 2 * nz // 3, STRIP, 128), f32),
                pltpu.VMEM((ngy, 1, 128), f32),
                pltpu.VMEM((ny * nz, 1, 128), f32),
                pltpu.VMEM((2, 1, 128), f32),
                dma((10,)),
                dma((8,)),
                dma((8,)),
                dma((nz - 2 * nz // 3,)),
                dma((nz - 2 * nz // 3,)),
                dma((6,)),
            ],
            compiler_params=pltpu.CompilerParams(collective_id=0, has_side_effects=True, vmem_limit_bytes=16 * 1024 * 1024),
            name="picard",
        )(*[pltpu.with_memory_space_constraint(a, pltpu.HBM) for a in args])

    both = P(None, "gx", "gy")
    one = P("gx", "gy")
    return jax.shard_map(
        body,
        mesh=mesh,
        in_specs=(both, both, one, one, one, one, one, one, one, one),
        out_specs=(both, one),
        check_vma=False,
    )


def solution(mesh):
    return build(mesh, 8, 12)
```

```python
import functools

import jax
import jax.numpy as jnp
from jax import lax
from jax.experimental import pallas as pl
from jax.experimental.pallas import tpu as pltpu
from jax.sharding import PartitionSpec as P

MESH = pl.DeviceIdType.MESH

M_U, M_V, H_U, H_V, M_O, H_O, B_I, B_O, TURN = range(9)
DEPTH = {M_U: 3, M_V: 3, M_O: 3, H_U: 2, H_V: 2, H_O: 2, B_I: 2, B_O: 2, TURN: 1}
HALVES = ((M_U, M_V, H_U, H_V), (M_O, H_O, B_I, B_O, TURN))
TILES = ((M_U, M_V, H_U), (M_O, H_V, H_O, TURN), (B_I, B_O))
PACK = 24
STRIP = PACK + 16
HUBS = 4
ROWS = 64
COLS = 256
EXT_ROWS = ROWS + 8
EXT_COLS = COLS + 128


def iota(shape, dim):
    return lax.broadcasted_iota(jnp.int32, shape, dim)


def roll(x, by, dim):
    size = x.shape[dim]
    return x if by % size == 0 else pltpu.roll(x, by % size, dim)


def columns():
    for half, fields in enumerate(HALVES):
        at = 0
        for f in fields:
            yield half, f, at, DEPTH[f]
            at += 2 * DEPTH[f]


def packed_rows():
    for t, fields in enumerate(TILES):
        at = 0
        for f in fields:
            yield t, f, at, DEPTH[f]
            at += DEPTH[f]


def northern_rows():
    row, lane = iota((PACK, 128), 0), iota((PACK, 128), 1)
    step = jnp.full((PACK, 128), -1, jnp.int32)
    for half, _, at, n in columns():
        here = (lane < 64) if half == 0 else (lane >= 64)
        for k in range(n):
            step = jnp.where(jnp.logical_and(here, row == at + n + k), k, step)
    return step


def corners(turned):
    lane = lax.rem(iota((8, 128), 1) + 2, 64)
    first, second, third = [roll(turned[8 * t : 8 * t + 8], 4 * t, 1) for t in range(3)]
    return jnp.where(lane < 4, first, jnp.where(lane < 8, second, third))


def from_corners(tile):
    return jnp.concatenate([roll(tile, -4 * t, 1) for t in range(3)], axis=0)


def around(q):
    rows, cols = q.shape
    return (
        pltpu.roll(q, 1, 0) + pltpu.roll(q, rows - 1, 0) + pltpu.roll(q, 1, 1) + pltpu.roll(q, cols - 1, 1)
    )


def inner_block(x):
    return x[:ROWS, :COLS]


def kernel(
    sizes,
    ice_rhs,
    ice_guess,
    ocean_rhs,
    ocean_guess,
    ice_diag,
    ice_visc,
    coriolis,
    depth_factor,
    wet_mask,
    ice_mask,
    velocity,
    level,
    v_rhs,
    v_guess,
    v_orhs,
    v_oguess,
    v_diag,
    v_visc,
    v_cor,
    v_depth,
    v_wet,
    v_ice,
    fields,
    local,
    zonal_out,
    zonal_in,
    merid_out,
    corner_out,
    north_in,
    south_in,
    post_in,
    seam_in,
    seam_corner,
    sum_gy,
    sum_plane,
    result,
    load_sems,
    halo_send,
    halo_recv,
    post_send,
    post_recv,
    seam_send,
    seam_recv,
    sum_sems,
):
    ny, nz, ngy = sizes
    ngx = ny * nz
    gx = lax.axis_index("gx")
    gy = lax.axis_index("gy")
    yy = gx // nz
    zz = lax.rem(gx, nz)
    top = gy == ngy - 1
    bottom = gy == 0

    loads = []
    for i, (src, dst) in enumerate(
        (
            (ice_rhs, v_rhs),
            (ice_guess, v_guess),
            (ocean_rhs, v_orhs),
            (ocean_guess, v_oguess),
            (ice_diag, v_diag),
            (ice_visc, v_visc),
            (coriolis, v_cor),
            (depth_factor, v_depth),
            (wet_mask, v_wet),
            (ice_mask, v_ice),
        )
    ):
        loads.append(pltpu.make_async_copy(src, dst, load_sems.at[i]))

    def wrap(x):
        return lax.rem(x + ngx, ngx)

    def north_of(step):
        there = wrap(gx + step)
        return jnp.where(top, ngx - 1 - there, there), jnp.where(top, gy, gy + 1)

    def south_of(step):
        return wrap(gx + step), jnp.where(bottom, gy, gy - 1)

    east = (wrap(gx + 1), gy)
    west = (wrap(gx - 1), gy)
    norths = [north_of(step) for step in (0, 1, -1)]
    souths = [south_of(step) for step in (0, 1, -1)]
    gy_peers = [lax.rem(gy + d, ngy) for d in range(1, ngy)]
    nhub = min(HUBS, nz - 1)
    hubs = [y * nz + z for z in range(nhub) for y in range(ny)]
    is_hub = zz < nhub
    later = [z for z in range(nhub, nz)]

    barrier = pltpu.get_barrier_semaphore()

    def greet(device):
        pl.semaphore_signal(barrier, inc=1, device_id=device, device_id_type=MESH)

    half_z, far_z = nz // 2, 3 * nz // 4
    posts = {}
    for z in range(half_z, nz):
        posts.setdefault(0 if z >= far_z else half_z - 1 - (z - half_z) % 2, []).append(z)
    post_plane = gy == ngy - 2

    def is_late(g):
        return lax.rem(g, nz) >= half_z

    def post_of(g):
        z = lax.rem(g, nz)
        far = z >= far_z
        at = jnp.where(far, 0, half_z - 1 - lax.rem(z + nz - half_z, 2))
        return g - z + at, jnp.where(far, z - far_z, (z - half_z) // 2)

    def mirrors(g):
        return [ngx - 1 - wrap(g + step) for step in (0, 1, -1)]

    late = is_late(gx)
    seam_source = jnp.logical_and(top, zz == 0)
    seam_post = jnp.logical_and(post_plane, zz == 0)
    seam_target = jnp.logical_and(top, zz == nz - 1)
    seam_diagonal = jnp.logical_and(post_plane, zz == nz - 1)
    mirror_self = [
        jnp.logical_and(jnp.logical_and(top, jnp.logical_not(late)), norths[k][0] == gx) for k in range(3)
    ]

    for copy in loads:
        copy.start()

    @pl.when(jnp.logical_and(top, late))
    def _():
        greet((post_of(gx)[0], gy - 1))

    for k in range(3):

        elsewhere = jnp.logical_or(jnp.logical_and(top, late), mirror_self[k])
        if k == 1:
            elsewhere = jnp.logical_or(elsewhere, seam_diagonal)

        @pl.when(jnp.logical_not(elsewhere))
        def _():
            greet(norths[k])

    @pl.when(seam_diagonal)
    def _():
        greet((gx - zz, gy))

    @pl.when(seam_post)
    def _():
        greet((wrap(gx + nz), gy + 1))

    @pl.when(jnp.logical_not(seam_target))
    def _():
        greet(east)

    greet(west)
    for p in gy_peers:
        greet((gx, p))

    @pl.when(jnp.logical_not(bottom))
    def _():
        for device in souths:
            greet(device)

    for at, served in posts.items():

        @pl.when(jnp.logical_and(post_plane, zz == at))
        def _():
            for z in served:
                for g in mirrors(yy * nz + z):
                    greet((g, gy + 1))

    @pl.when(is_hub)
    def _():
        for d in range(1, ngx):
            greet((lax.rem(gx + d, ngx), gy))

    for copy in loads:
        copy.wait()

    wet = v_wet[...].astype(jnp.float32)
    active = wet * v_ice[...].astype(jnp.float32)
    visc = v_visc[...]
    depth = v_depth[...]
    d_i = active * (v_diag[...] + 4.0 * visc * visc) + 1.0 - active
    d_o = wet * (1.0 + 4.0 * depth * depth) + 1.0 - wet
    p_i = 1.0 / d_i
    p_o = 1.0 / d_o
    r_i = active * visc
    r_o = wet * depth
    s_i = r_i * p_i
    s_o = r_o * p_o
    c = active * v_cor[...]
    g_u = v_guess[0]
    g_v = v_guess[1]
    g_o = v_oguess[...]
    h_u = v_rhs[0] - d_i * g_u + c * g_v
    h_v = v_rhs[1] - d_i * g_v - c * g_u
    h_o = v_orhs[...] - d_o * g_o
    own = {
        M_U: r_i * g_u,
        M_V: r_i * g_v,
        M_O: r_o * g_o,
        H_U: s_i * h_u,
        H_V: s_i * h_v,
        H_O: s_o * h_o,
        B_I: r_i * s_i,
        B_O: r_o * s_o,
        TURN: c * p_i,
    }
    for k, value in enumerate((h_u, h_v, h_o, r_i, r_o, p_i, p_o)):
        local[k] = value
    for f in range(9):
        fields[f, 0:ROWS, 0:COLS] = own[f]

    sub = iota((8, COLS), 0)
    eastward = [jnp.zeros((8, COLS), jnp.float32)] * len(TILES)
    westward = [jnp.zeros((8, COLS), jnp.float32)] * len(TILES)
    for t, f, at, n in packed_rows():
        eastward[t] = jnp.where(
            jnp.logical_and(sub >= 8 - at - n, sub < 8 - at), roll(own[f][ROWS - 8 : ROWS], -at, 0), eastward[t]
        )
        westward[t] = jnp.where(jnp.logical_and(sub >= at, sub < at + n), roll(own[f][0:8], at, 0), westward[t])
    for t in range(len(TILES)):
        zonal_out[0, t] = eastward[t]
        zonal_out[1, t] = westward[t]

    lane = iota((ROWS, 128), 1)
    halves = [jnp.zeros((ROWS, 128), jnp.float32)] * 2
    for half, f, at, n in columns():
        edge = jnp.where(lane < 64, own[f][:, 0:128], own[f][:, COLS - 128 : COLS])
        halves[half] = jnp.where(
            jnp.logical_and(lane >= at, lane < at + 2 * n), roll(edge, at + n, 1), halves[half]
        )
    turned = jnp.transpose(jnp.concatenate(halves, axis=0))[0:PACK]
    merid_out[0] = turned
    merid_out[1] = turned
    corner_out[0] = corners(turned)
    corner_out[1] = corners(turned)

    @pl.when(top)
    def _():
        step = northern_rows()
        flipped = jnp.where(
            step == 0, roll(turned, 1, 0), jnp.where(step == 1, roll(turned, 3, 0), roll(turned, 5, 0))
        )
        swap = jnp.where(
            (iota((128, 128), 0) ^ iota((128, 128), 1)) == 63, 1.0, 0.0
        ).astype(jnp.float32)
        mirrored = jnp.dot(
            flipped, swap, precision=lax.Precision.HIGHEST, preferred_element_type=jnp.float32
        )
        mirrored = jnp.where(iota((PACK, 128), 1) < 64, -mirrored, mirrored)
        merid_out[0] = mirrored
        corner_out[0] = corners(mirrored)

    @pl.when(bottom)
    def _():
        south_in[...] = jnp.zeros((STRIP, 128), jnp.float32)

    expected = len(hubs) + ngy - 1 + 2 + 3 + jnp.where(bottom, 0, 3) - jnp.where(is_hub, 1, 0)
    for k in range(3):
        expected = expected - jnp.where(mirror_self[k], 1, 0)
    for at, served in posts.items():
        expected = expected + jnp.where(jnp.logical_and(post_plane, zz == at), len(served), 0)
    expected = expected + jnp.where(seam_post, 1, 0) - jnp.where(seam_source, 1, 0)
    pl.semaphore_wait(barrier, expected)

    def remote(src, dst, sent, got, device):
        return pltpu.make_async_remote_copy(
            src_ref=src,
            dst_ref=dst,
            send_sem=halo_send.at[sent],
            recv_sem=halo_recv.at[got],
            device_id=device,
            device_id_type=MESH,
        )

    parts = [pl.ds(0, PACK), pl.ds(PACK, 8), pl.ds(PACK + 8, 8)]
    opposite = (0, 2, 1)
    sources = [[merid_out.at[i], corner_out.at[i], corner_out.at[i]] for i in range(2)]
    fold = [remote(sources[0][k], north_in.at[parts[k]], k, k, norths[k]) for k in range(3)]
    up = [
        remote(sources[0][k], south_in.at[parts[opposite[k]]], k, 3 + opposite[k], norths[k])
        for k in range(3)
    ]
    down = [
        remote(sources[1][k], north_in.at[parts[opposite[k]]], 3 + k, opposite[k], souths[k])
        for k in range(3)
    ]

    def to_post(k):
        post, slot = post_of(norths[k][0])
        return pltpu.make_async_remote_copy(
            src_ref=sources[0][k],
            dst_ref=post_in.at[slot, parts[k]],
            send_sem=halo_send.at[k],
            recv_sem=post_recv.at[slot],
            device_id=(post, gy - 1),
            device_id_type=MESH,
        )

    to_east = remote(zonal_out.at[0], zonal_in.at[0], 6, 6, east)
    to_west = remote(zonal_out.at[1], zonal_in.at[1], 7, 7, west)

    def from_seam(src, dst, i, recv, there):
        return pltpu.make_async_remote_copy(
            src_ref=src,
            dst_ref=dst,
            send_sem=seam_send.at[i],
            recv_sem=halo_recv.at[recv],
            device_id=(gx - zz + nz - 1, there),
            device_id_type=MESH,
        )

    seam_rows = from_seam(seam_in, zonal_in.at[1], 0, 7, gy + 1)
    seam_tile = from_seam(seam_corner, north_in.at[parts[1]], 1, 1, gy)

    for at, served in posts.items():

        @pl.when(jnp.logical_and(post_plane, zz == at))
        def _():
            for slot, z in enumerate(served):
                strip = post_in.at[slot]
                pltpu.make_async_copy(strip, strip, post_recv.at[slot]).wait()
                pltpu.make_async_remote_copy(
                    src_ref=strip,
                    dst_ref=north_in,
                    send_sem=post_send.at[slot],
                    recv_sem=halo_recv.at[0],
                    device_id=(yy * nz + z, gy + 1),
                    device_id_type=MESH,
                ).start()
            if at == 0:
                pltpu.make_async_copy(seam_in, seam_in, seam_recv.at[0]).wait()
                seam_rows.start()
                pltpu.make_async_copy(seam_corner, seam_corner, seam_recv.at[1]).wait()
                seam_tile.start()

    target_late = [is_late(norths[k][0]) for k in range(3)]
    for k in range(3):

        @pl.when(jnp.logical_and(top, target_late[k]))
        def _():
            to_post(k).start()

        @pl.when(
            jnp.logical_and(
                jnp.logical_and(top, jnp.logical_not(target_late[k])), jnp.logical_not(mirror_self[k])
            )
        )
        def _():
            fold[k].start()

        @pl.when(mirror_self[k])
        def _():
            north_in[PACK + 8 * max(k - 1, 0) : PACK + 8 * max(k - 1, 0) + 8] = corner_out[0]

    @pl.when(jnp.logical_not(top))
    def _():
        for copy in up:
            copy.start()

    @pl.when(jnp.logical_not(bottom))
    def _():
        for copy in down[0:2]:
            copy.start()

    def to_seam(src, dst, sent, i):
        return pltpu.make_async_remote_copy(
            src_ref=src,
            dst_ref=dst,
            send_sem=halo_send.at[sent],
            recv_sem=seam_recv.at[i],
            device_id=(wrap(gx - nz), gy - 1),
            device_id_type=MESH,
        )

    @pl.when(seam_source)
    def _():
        to_seam(zonal_out.at[1], seam_in, 7, 0).start()
        to_seam(corner_out.at[1], seam_corner, 5, 1).start()

    @pl.when(jnp.logical_not(seam_source))
    def _():
        to_west.start()

    @pl.when(jnp.logical_not(jnp.logical_or(bottom, seam_source)))
    def _():
        down[2].start()

    to_east.start()

    to_east.wait_recv()
    to_west.wait_recv()

    for t, f, at, n in packed_rows():
        fields[f, ROWS:EXT_ROWS, 0:COLS] = jnp.where(
            sub < 4, roll(zonal_in[1, t], -at, 0), roll(zonal_in[0, t], at, 0)
        )

    def arrived(k, dst):
        pltpu.make_async_copy(dst, dst, halo_recv.at[k]).wait()

    @pl.when(jnp.logical_and(top, late))
    def _():
        arrived(0, north_in)

    for k in range(3):

        @pl.when(jnp.logical_not(jnp.logical_or(jnp.logical_and(top, late), mirror_self[k])))
        def _():
            arrived(k, north_in.at[parts[k]])

        @pl.when(jnp.logical_not(bottom))
        def _():
            arrived(3 + k, south_in.at[parts[k]])

    northern = northern_rows() >= 0
    plane = jnp.where(northern, north_in[0:PACK], south_in[0:PACK])
    from_e, from_w = [
        jnp.where(northern, from_corners(north_in[at : at + 8]), from_corners(south_in[at : at + 8]))
        for at in (PACK, PACK + 8)
    ]
    lane = iota((PACK, 128), 1)
    pad = jnp.zeros((128 - PACK, 128), jnp.float32)
    backs = []
    for half in range(2):
        if half == 0:
            center, right, left = plane, roll(from_e, 64, 1), roll(from_w, 8, 1)
        else:
            center, right, left = roll(plane, 64, 1), from_e, roll(from_w, 72, 1)
        merged = jnp.where(lane < 64, center, jnp.where(lane < 68, right, left))
        backs.append(jnp.transpose(jnp.concatenate([merged, pad], axis=0))[0:EXT_ROWS])
    for half, f, at, n in columns():
        fields[f, :, COLS:EXT_COLS] = roll(backs[half], -(at + n), 1)

    b_i = fields[B_I]
    b_o = fields[B_O]
    turn = fields[TURN]
    t_in = inner_block(turn)
    h_u, h_v, h_o = local[0], local[1], local[2]
    r_i, r_o, p_i, p_o = local[3], local[4], local[5], local[6]
    nb_u = around(fields[M_U])
    nb_v = around(fields[M_V])
    nb_o = around(fields[M_O])
    s0_u = fields[H_U] + b_i * nb_u
    s0_v = fields[H_V] + b_i * nb_v
    s0_o = fields[H_O] + b_o * nb_o
    res_u = h_u + r_i * inner_block(nb_u)
    res_v = h_v + r_i * inner_block(nb_v)
    res_o = h_o + r_o * inner_block(nb_o)
    nb_u = around(s0_u)
    nb_v = around(s0_v)
    nb_o = around(s0_o)
    s1_u = b_i * nb_u + turn * s0_v
    s1_v = b_i * nb_v - turn * s0_u
    s1_o = b_o * nb_o
    n1_u = r_i * inner_block(nb_u) + t_in * res_v
    n1_v = r_i * inner_block(nb_v) - t_in * res_u
    n1_o = r_o * inner_block(nb_o)
    n2_u = r_i * inner_block(around(s1_u)) + t_in * n1_v
    n2_v = r_i * inner_block(around(s1_v)) - t_in * n1_u
    n2_o = r_o * inner_block(around(s1_o))
    a_u, a_v, a_o = res_u - n1_u, res_v - n1_v, res_o - n1_o
    e_u, e_v, e_o = n1_u - n2_u, n1_v - n2_v, n1_o - n2_o
    z_o = p_o * res_o
    x_o = p_o * n1_o
    products = [
        a_u * a_u + a_v * a_v,
        a_u * e_u + a_v * e_v,
        e_u * e_u + e_v * e_v,
        a_u * res_u + a_v * res_v,
        e_u * res_u + e_v * res_v,
        z_o * a_o,
        x_o * a_o,
        x_o * e_o,
        z_o * res_o,
        x_o * res_o,
    ]
    local[0] = p_i * res_u
    local[1] = p_i * res_v
    local[2] = z_o
    local[3] = p_i * n1_u
    local[4] = p_i * n1_v
    local[5] = x_o

    row = iota((16, 128), 0)
    sums = jnp.zeros((16, 128), jnp.float32)
    for k, product in enumerate(products):
        half = product[:, 0:128] + product[:, 128:256]
        sums = jnp.where(row == k, jnp.sum(half, axis=0, keepdims=True), sums)
    sums = jnp.sum(sums, axis=1, keepdims=True)
    mine = jnp.sum(jnp.where(row == iota((16, 128), 1), sums, 0.0), axis=0, keepdims=True)

    def rows_of(slots, count, sem):
        return pltpu.make_async_copy(slots.at[pl.ds(0, count)], slots.at[pl.ds(0, count)], sem)

    def send_row(slots, at, dst, dst_at, send, recv, device):
        pltpu.make_async_remote_copy(
            src_ref=slots.at[at],
            dst_ref=dst.at[dst_at],
            send_sem=sum_sems.at[send],
            recv_sem=sum_sems.at[recv],
            device_id=device,
            device_id_type=MESH,
        ).start()

    sum_gy[gy] = mine
    for p in gy_peers:
        send_row(sum_gy, gy, sum_gy, gy, 0, 1, (gx, p))
    rows_of(sum_gy, ngy - 1, sum_sems.at[1]).wait()
    total = sum_gy[0]
    for k in range(1, ngy):
        total = total + sum_gy[k]

    sum_plane[gx] = total
    for hub in hubs:

        @pl.when(gx != hub)
        def _():
            send_row(sum_plane, gx, sum_plane, gx, 2, 3, (hub, gy))

    @pl.when(is_hub)
    def _():
        rows_of(sum_plane, ngx - 1, sum_sems.at[3]).wait()
        whole = sum_plane[0]
        for k in range(1, ngx):
            whole = whole + sum_plane[k]
        result[0] = whole
        result[1] = whole
        for z in later:

            @pl.when(zz == nhub - 1)
            def _():
                send_row(result, 0, result, 1, 4, 5, (yy * nz + z, gy))

    @pl.when(jnp.logical_not(is_hub))
    def _():
        rows_of(result, 1, sum_sems.at[5]).wait()

    total = result[1]

    def item(k):
        return total[0:1, k : k + 1]

    def solve(k11, k12, k22, k1, k2):
        scale = 1.0 / item(k11)
        a12, a22 = item(k12) * scale, item(k22) * scale
        f1, f2 = item(k1) * scale, item(k2) * scale
        det = 1.0 / (a22 - a12 * a12)
        return (a22 * f1 - a12 * f2) * det, (f2 - a12 * f1) * det

    c1, c2 = solve(0, 1, 2, 3, 4)
    d1, d2 = solve(5, 6, 7, 8, 9)
    velocity[0] = v_guess[0] + c1 * local[0] + c2 * local[3]
    velocity[1] = v_guess[1] + c1 * local[1] + c2 * local[4]
    level[...] = v_oguess[...] + d1 * local[2] + d2 * local[5]

    for k in range(3):

        @pl.when(jnp.logical_and(top, jnp.logical_not(mirror_self[k])))
        def _():
            fold[k].wait_send()

    for at, served in posts.items():

        @pl.when(jnp.logical_and(post_plane, zz == at))
        def _():
            for slot, _ in enumerate(served):
                pltpu.make_async_copy(post_in.at[slot], post_in.at[slot], post_send.at[slot]).wait()
            if at == 0:
                seam_rows.wait_send()
                seam_tile.wait_send()

    @pl.when(jnp.logical_not(top))
    def _():
        for copy in up:
            copy.wait_send()

    @pl.when(jnp.logical_not(bottom))
    def _():
        for k in range(3):
            down[k].wait_send()

    to_east.wait_send()
    to_west.wait_send()
    rows_of(sum_gy, ngy - 1, sum_sems.at[0]).wait()

    @pl.when(is_hub)
    def _():
        rows_of(sum_plane, len(hubs) - 1, sum_sems.at[2]).wait()

    @pl.when(jnp.logical_not(is_hub))
    def _():
        rows_of(sum_plane, len(hubs), sum_sems.at[2]).wait()

    @pl.when(zz == nhub - 1)
    def _():
        rows_of(sum_plane, len(later), sum_sems.at[4]).wait()


def build(mesh, ny, nz, interpret=False):
    ngy = mesh.shape["gy"]
    f32 = jnp.float32
    block = pltpu.VMEM((ROWS, COLS), f32)
    pair = pltpu.VMEM((2, ROWS, COLS), f32)
    whole = pltpu.VMEM((ROWS, COLS), jnp.int32)
    dma = pltpu.SemaphoreType.DMA
    slots = max(nz - 3 * nz // 4, (3 * nz // 4 - nz // 2 + 1) // 2)

    def body(*args):
        return pl.pallas_call(
            functools.partial(kernel, (ny, nz, ngy)),
            out_shape=(
                pltpu.VMEM((2, ROWS, COLS), f32),
                pltpu.VMEM((ROWS, COLS), f32),
            ),
            in_specs=[pl.BlockSpec(memory_space=pl.ANY)] * 10,
            out_specs=(pl.BlockSpec(memory_space=pltpu.VMEM), pl.BlockSpec(memory_space=pltpu.VMEM)),
            scratch_shapes=[
                pair,
                pair,
                block,
                block,
                block,
                block,
                block,
                block,
                whole,
                whole,
                pltpu.VMEM((9, EXT_ROWS, EXT_COLS), f32),
                pltpu.VMEM((7, ROWS, COLS), f32),
                pltpu.VMEM((2, 3, 8, COLS), f32),
                pltpu.VMEM((2, 3, 8, COLS), f32),
                pltpu.VMEM((2, PACK, 128), f32),
                pltpu.VMEM((2, 8, 128), f32),
                pltpu.VMEM((STRIP, 128), f32),
                pltpu.VMEM((STRIP, 128), f32),
                pltpu.VMEM((slots, STRIP, 128), f32),
                pltpu.VMEM((3, 8, COLS), f32),
                pltpu.VMEM((8, 128), f32),
                pltpu.VMEM((ngy, 1, 128), f32),
                pltpu.VMEM((ny * nz, 1, 128), f32),
                pltpu.VMEM((2, 1, 128), f32),
                dma((10,)),
                dma((8,)),
                dma((8,)),
                dma((slots,)),
                dma((slots,)),
                dma((2,)),
                dma((2,)),
                dma((6,)),
            ],
            compiler_params=pltpu.CompilerParams(collective_id=0, has_side_effects=True, vmem_limit_bytes=16 * 1024 * 1024),
            name="picard",
        )(*[pltpu.with_memory_space_constraint(a, pltpu.HBM) for a in args])

    both = P(None, "gx", "gy")
    one = P("gx", "gy")
    return jax.shard_map(
        body,
        mesh=mesh,
        in_specs=(both, both, one, one, one, one, one, one, one, one),
        out_specs=(both, one),
        check_vma=False,
    )


def solution(mesh):
    return build(mesh, 8, 12)
```

```python
import functools

import jax
import jax.numpy as jnp
from jax import lax
from jax.experimental import pallas as pl
from jax.experimental.pallas import tpu as pltpu
from jax.sharding import PartitionSpec as P

MESH = pl.DeviceIdType.MESH

M_U, M_V, H_U, H_V, M_O, H_O, B_I, B_O, TURN = range(9)
DEPTH = {M_U: 3, M_V: 3, M_O: 3, H_U: 2, H_V: 2, H_O: 2, B_I: 2, B_O: 2, TURN: 1}
HALVES = ((M_U, M_V, H_U, H_V), (M_O, H_O, B_I, B_O, TURN))
TILES = ((M_U, M_V, H_U), (M_O, H_V, H_O, TURN), (B_I, B_O))
PACK = 24
STRIP = PACK + 16
HUBS = 4
ROWS = 64
COLS = 256
EXT_ROWS = ROWS + 8
EXT_COLS = COLS + 128


def iota(shape, dim):
    return lax.broadcasted_iota(jnp.int32, shape, dim)


def roll(x, by, dim):
    size = x.shape[dim]
    return x if by % size == 0 else pltpu.roll(x, by % size, dim)


def columns():
    for half, fields in enumerate(HALVES):
        at = 0
        for f in fields:
            yield half, f, at, DEPTH[f]
            at += 2 * DEPTH[f]


def packed_rows():
    for t, fields in enumerate(TILES):
        at = 0
        for f in fields:
            yield t, f, at, DEPTH[f]
            at += DEPTH[f]


def northern_rows():
    row, lane = iota((PACK, 128), 0), iota((PACK, 128), 1)
    step = jnp.full((PACK, 128), -1, jnp.int32)
    for half, _, at, n in columns():
        here = (lane < 64) if half == 0 else (lane >= 64)
        for k in range(n):
            step = jnp.where(jnp.logical_and(here, row == at + n + k), k, step)
    return step


def corners(turned):
    lane = lax.rem(iota((8, 128), 1) + 2, 64)
    first, second, third = [roll(turned[8 * t : 8 * t + 8], 4 * t, 1) for t in range(3)]
    return jnp.where(lane < 4, first, jnp.where(lane < 8, second, third))


def from_corners(tile):
    return jnp.concatenate([roll(tile, -4 * t, 1) for t in range(3)], axis=0)


def around(q):
    rows, cols = q.shape
    return (
        pltpu.roll(q, 1, 0) + pltpu.roll(q, rows - 1, 0) + pltpu.roll(q, 1, 1) + pltpu.roll(q, cols - 1, 1)
    )


def inner_block(x):
    return x[:ROWS, :COLS]


def kernel(
    sizes,
    ice_rhs,
    ice_guess,
    ocean_rhs,
    ocean_guess,
    ice_diag,
    ice_visc,
    coriolis,
    depth_factor,
    wet_mask,
    ice_mask,
    velocity,
    level,
    v_rhs,
    v_guess,
    v_orhs,
    v_oguess,
    v_diag,
    v_visc,
    v_cor,
    v_depth,
    v_wet,
    v_ice,
    fields,
    local,
    zonal_out,
    zonal_in,
    merid_out,
    corner_out,
    north_in,
    south_in,
    post_in,
    sum_gy,
    sum_plane,
    result,
    load_sems,
    halo_send,
    halo_recv,
    post_send,
    post_recv,
    sum_sems,
):
    ny, nz, ngy = sizes
    ngx = ny * nz
    gx = lax.axis_index("gx")
    gy = lax.axis_index("gy")
    yy = gx // nz
    zz = lax.rem(gx, nz)
    top = gy == ngy - 1
    bottom = gy == 0

    loads = []
    for i, (src, dst) in enumerate(
        (
            (ice_rhs, v_rhs),
            (ice_guess, v_guess),
            (ocean_rhs, v_orhs),
            (ocean_guess, v_oguess),
            (ice_diag, v_diag),
            (ice_visc, v_visc),
            (coriolis, v_cor),
            (depth_factor, v_depth),
            (wet_mask, v_wet),
            (ice_mask, v_ice),
        )
    ):
        loads.append(pltpu.make_async_copy(src, dst, load_sems.at[i]))

    def wrap(x):
        return lax.rem(x + ngx, ngx)

    def north_of(step):
        there = wrap(gx + step)
        return jnp.where(top, ngx - 1 - there, there), jnp.where(top, gy, gy + 1)

    def south_of(step):
        return wrap(gx + step), jnp.where(bottom, gy, gy - 1)

    east = (wrap(gx + 1), gy)
    west = (wrap(gx - 1), gy)
    norths = [north_of(step) for step in (0, 1, -1)]
    souths = [south_of(step) for step in (0, 1, -1)]
    gy_peers = [lax.rem(gy + d, ngy) for d in range(1, ngy)]
    nhub = min(HUBS, nz - 1)
    hubs = [y * nz + z for z in range(nhub) for y in range(ny)]
    is_hub = zz < nhub
    later = [z for z in range(nhub, nz)]

    barrier = pltpu.get_barrier_semaphore()

    def greet(device):
        pl.semaphore_signal(barrier, inc=1, device_id=device, device_id_type=MESH)

    far_z = 2 * nz // 3
    posts = {}
    for z in range(nz // 2, nz):
        posts.setdefault(0 if z >= far_z else nz - 1 - z, []).append(z)

    def is_late(g):
        return 2 * lax.rem(g, nz) >= nz

    def post_of(g):
        z = lax.rem(g, nz)
        far = z >= far_z
        return g - z + jnp.where(far, 0, nz - 1 - z), jnp.where(far, z - far_z, 0)

    def mirrors(g):
        return [ngx - 1 - wrap(g + step) for step in (0, 1, -1)]

    late = is_late(gx)
    mirror_self = [
        jnp.logical_and(jnp.logical_and(top, jnp.logical_not(late)), norths[k][0] == gx) for k in range(3)
    ]

    for copy in loads:
        copy.start()

    @pl.when(jnp.logical_and(top, late))
    def _():
        greet((post_of(gx)[0], gy))

    for k in range(3):

        @pl.when(jnp.logical_not(jnp.logical_or(jnp.logical_and(top, late), mirror_self[k])))
        def _():
            greet(norths[k])

    greet(east)
    greet(west)
    for p in gy_peers:
        greet((gx, p))

    @pl.when(jnp.logical_not(bottom))
    def _():
        for device in souths:
            greet(device)

    for at, served in posts.items():

        @pl.when(jnp.logical_and(top, zz == at))
        def _():
            for z in served:
                for g in mirrors(yy * nz + z):
                    greet((g, gy))

    @pl.when(is_hub)
    def _():
        for d in range(1, ngx):
            greet((lax.rem(gx + d, ngx), gy))

    for copy in loads:
        copy.wait()

    wet = v_wet[...].astype(jnp.float32)
    active = wet * v_ice[...].astype(jnp.float32)
    visc = v_visc[...]
    depth = v_depth[...]
    d_i = active * (v_diag[...] + 4.0 * visc * visc) + 1.0 - active
    d_o = wet * (1.0 + 4.0 * depth * depth) + 1.0 - wet
    p_i = 1.0 / d_i
    p_o = 1.0 / d_o
    r_i = active * visc
    r_o = wet * depth
    s_i = r_i * p_i
    s_o = r_o * p_o
    c = active * v_cor[...]
    g_u = v_guess[0]
    g_v = v_guess[1]
    g_o = v_oguess[...]
    h_u = v_rhs[0] - d_i * g_u + c * g_v
    h_v = v_rhs[1] - d_i * g_v - c * g_u
    h_o = v_orhs[...] - d_o * g_o
    own = {
        M_U: r_i * g_u,
        M_V: r_i * g_v,
        M_O: r_o * g_o,
        H_U: s_i * h_u,
        H_V: s_i * h_v,
        H_O: s_o * h_o,
        B_I: r_i * s_i,
        B_O: r_o * s_o,
        TURN: c * p_i,
    }
    for k, value in enumerate((h_u, h_v, h_o, r_i, r_o, p_i, p_o)):
        local[k] = value
    for f in range(9):
        fields[f, 0:ROWS, 0:COLS] = own[f]

    sub = iota((8, COLS), 0)
    eastward = [jnp.zeros((8, COLS), jnp.float32)] * len(TILES)
    westward = [jnp.zeros((8, COLS), jnp.float32)] * len(TILES)
    for t, f, at, n in packed_rows():
        eastward[t] = jnp.where(
            jnp.logical_and(sub >= 8 - at - n, sub < 8 - at), roll(own[f][ROWS - 8 : ROWS], -at, 0), eastward[t]
        )
        westward[t] = jnp.where(jnp.logical_and(sub >= at, sub < at + n), roll(own[f][0:8], at, 0), westward[t])
    for t in range(len(TILES)):
        zonal_out[0, t] = eastward[t]
        zonal_out[1, t] = westward[t]

    lane = iota((ROWS, 128), 1)
    halves = [jnp.zeros((ROWS, 128), jnp.float32)] * 2
    for half, f, at, n in columns():
        edge = jnp.where(lane < 64, own[f][:, 0:128], own[f][:, COLS - 128 : COLS])
        halves[half] = jnp.where(
            jnp.logical_and(lane >= at, lane < at + 2 * n), roll(edge, at + n, 1), halves[half]
        )
    turned = jnp.transpose(jnp.concatenate(halves, axis=0))[0:PACK]
    merid_out[0] = turned
    merid_out[1] = turned
    corner_out[0] = corners(turned)
    corner_out[1] = corners(turned)

    @pl.when(top)
    def _():
        step = northern_rows()
        flipped = jnp.where(
            step == 0, roll(turned, 1, 0), jnp.where(step == 1, roll(turned, 3, 0), roll(turned, 5, 0))
        )
        swap = jnp.where(
            (iota((128, 128), 0) ^ iota((128, 128), 1)) == 63, 1.0, 0.0
        ).astype(jnp.float32)
        mirrored = jnp.dot(
            flipped, swap, precision=lax.Precision.HIGHEST, preferred_element_type=jnp.float32
        )
        mirrored = jnp.where(iota((PACK, 128), 1) < 64, -mirrored, mirrored)
        merid_out[0] = mirrored
        corner_out[0] = corners(mirrored)

    @pl.when(bottom)
    def _():
        south_in[...] = jnp.zeros((STRIP, 128), jnp.float32)

    expected = len(hubs) + ngy - 1 + 2 + 3 + jnp.where(bottom, 0, 3) - jnp.where(is_hub, 1, 0)
    for k in range(3):
        expected = expected - jnp.where(mirror_self[k], 1, 0)
    for at, served in posts.items():
        expected = expected + jnp.where(jnp.logical_and(top, zz == at), len(served), 0)
    pl.semaphore_wait(barrier, expected)

    def remote(src, dst, sent, got, device):
        return pltpu.make_async_remote_copy(
            src_ref=src,
            dst_ref=dst,
            send_sem=halo_send.at[sent],
            recv_sem=halo_recv.at[got],
            device_id=device,
            device_id_type=MESH,
        )

    parts = [pl.ds(0, PACK), pl.ds(PACK, 8), pl.ds(PACK + 8, 8)]
    opposite = (0, 2, 1)
    sources = [[merid_out.at[i], corner_out.at[i], corner_out.at[i]] for i in range(2)]
    fold = [remote(sources[0][k], north_in.at[parts[k]], k, k, norths[k]) for k in range(3)]
    up = [
        remote(sources[0][k], south_in.at[parts[opposite[k]]], k, 3 + opposite[k], norths[k])
        for k in range(3)
    ]
    down = [
        remote(sources[1][k], north_in.at[parts[opposite[k]]], 3 + k, opposite[k], souths[k])
        for k in range(3)
    ]

    def to_post(k):
        post, slot = post_of(norths[k][0])
        return pltpu.make_async_remote_copy(
            src_ref=sources[0][k],
            dst_ref=post_in.at[slot, parts[k]],
            send_sem=halo_send.at[k],
            recv_sem=post_recv.at[slot],
            device_id=(post, gy),
            device_id_type=MESH,
        )

    to_east = remote(zonal_out.at[0], zonal_in.at[0], 6, 6, east)
    to_west = remote(zonal_out.at[1], zonal_in.at[1], 7, 7, west)

    target_late = [is_late(norths[k][0]) for k in range(3)]
    for k in range(3):

        @pl.when(jnp.logical_and(top, target_late[k]))
        def _():
            to_post(k).start()

        @pl.when(
            jnp.logical_and(
                jnp.logical_and(top, jnp.logical_not(target_late[k])), jnp.logical_not(mirror_self[k])
            )
        )
        def _():
            fold[k].start()

        @pl.when(mirror_self[k])
        def _():
            north_in[PACK + 8 * max(k - 1, 0) : PACK + 8 * max(k - 1, 0) + 8] = corner_out[0]

    @pl.when(jnp.logical_not(top))
    def _():
        for copy in up:
            copy.start()

    @pl.when(jnp.logical_not(bottom))
    def _():
        for copy in down:
            copy.start()

    to_east.start()
    to_west.start()

    for at, served in posts.items():

        @pl.when(jnp.logical_and(top, zz == at))
        def _():
            for slot, z in enumerate(served):
                strip = post_in.at[slot]
                pltpu.make_async_copy(strip, strip, post_recv.at[slot]).wait()
                pltpu.make_async_remote_copy(
                    src_ref=strip,
                    dst_ref=north_in,
                    send_sem=post_send.at[slot],
                    recv_sem=halo_recv.at[0],
                    device_id=(yy * nz + z, gy),
                    device_id_type=MESH,
                ).start()

    to_east.wait_recv()
    to_west.wait_recv()

    for t, f, at, n in packed_rows():
        fields[f, ROWS:EXT_ROWS, 0:COLS] = jnp.where(
            sub < 4, roll(zonal_in[1, t], -at, 0), roll(zonal_in[0, t], at, 0)
        )

    def arrived(k, dst):
        pltpu.make_async_copy(dst, dst, halo_recv.at[k]).wait()

    @pl.when(jnp.logical_and(top, late))
    def _():
        arrived(0, north_in)

    for k in range(3):

        @pl.when(jnp.logical_not(jnp.logical_or(jnp.logical_and(top, late), mirror_self[k])))
        def _():
            arrived(k, north_in.at[parts[k]])

        @pl.when(jnp.logical_not(bottom))
        def _():
            arrived(3 + k, south_in.at[parts[k]])

    northern = northern_rows() >= 0
    plane = jnp.where(northern, north_in[0:PACK], south_in[0:PACK])
    from_e, from_w = [
        jnp.where(northern, from_corners(north_in[at : at + 8]), from_corners(south_in[at : at + 8]))
        for at in (PACK, PACK + 8)
    ]
    lane = iota((PACK, 128), 1)
    pad = jnp.zeros((128 - PACK, 128), jnp.float32)
    backs = []
    for half in range(2):
        if half == 0:
            center, right, left = plane, roll(from_e, 64, 1), roll(from_w, 8, 1)
        else:
            center, right, left = roll(plane, 64, 1), from_e, roll(from_w, 72, 1)
        merged = jnp.where(lane < 64, center, jnp.where(lane < 68, right, left))
        backs.append(jnp.transpose(jnp.concatenate([merged, pad], axis=0))[0:EXT_ROWS])
    for half, f, at, n in columns():
        fields[f, :, COLS:EXT_COLS] = roll(backs[half], -(at + n), 1)

    b_i = fields[B_I]
    b_o = fields[B_O]
    turn = fields[TURN]
    t_in = inner_block(turn)
    h_u, h_v, h_o = local[0], local[1], local[2]
    r_i, r_o, p_i, p_o = local[3], local[4], local[5], local[6]
    nb_u = around(fields[M_U])
    nb_v = around(fields[M_V])
    nb_o = around(fields[M_O])
    s0_u = fields[H_U] + b_i * nb_u
    s0_v = fields[H_V] + b_i * nb_v
    s0_o = fields[H_O] + b_o * nb_o
    res_u = h_u + r_i * inner_block(nb_u)
    res_v = h_v + r_i * inner_block(nb_v)
    res_o = h_o + r_o * inner_block(nb_o)
    nb_u = around(s0_u)
    nb_v = around(s0_v)
    nb_o = around(s0_o)
    s1_u = b_i * nb_u + turn * s0_v
    s1_v = b_i * nb_v - turn * s0_u
    s1_o = b_o * nb_o
    n1_u = r_i * inner_block(nb_u) + t_in * res_v
    n1_v = r_i * inner_block(nb_v) - t_in * res_u
    n1_o = r_o * inner_block(nb_o)
    n2_u = r_i * inner_block(around(s1_u)) + t_in * n1_v
    n2_v = r_i * inner_block(around(s1_v)) - t_in * n1_u
    n2_o = r_o * inner_block(around(s1_o))
    a_u, a_v, a_o = res_u - n1_u, res_v - n1_v, res_o - n1_o
    e_u, e_v, e_o = n1_u - n2_u, n1_v - n2_v, n1_o - n2_o
    z_o = p_o * res_o
    x_o = p_o * n1_o
    products = [
        a_u * a_u + a_v * a_v,
        a_u * e_u + a_v * e_v,
        e_u * e_u + e_v * e_v,
        a_u * res_u + a_v * res_v,
        e_u * res_u + e_v * res_v,
        z_o * a_o,
        x_o * a_o,
        x_o * e_o,
        z_o * res_o,
        x_o * res_o,
    ]
    local[0] = p_i * res_u
    local[1] = p_i * res_v
    local[2] = z_o
    local[3] = p_i * n1_u
    local[4] = p_i * n1_v
    local[5] = x_o

    row = iota((16, 128), 0)
    sums = jnp.zeros((16, 128), jnp.float32)
    for k, product in enumerate(products):
        half = product[:, 0:128] + product[:, 128:256]
        sums = jnp.where(row == k, jnp.sum(half, axis=0, keepdims=True), sums)
    sums = jnp.sum(sums, axis=1, keepdims=True)
    mine = jnp.sum(jnp.where(row == iota((16, 128), 1), sums, 0.0), axis=0, keepdims=True)

    def rows_of(slots, count, sem):
        return pltpu.make_async_copy(slots.at[pl.ds(0, count)], slots.at[pl.ds(0, count)], sem)

    def send_row(slots, at, dst, dst_at, send, recv, device):
        pltpu.make_async_remote_copy(
            src_ref=slots.at[at],
            dst_ref=dst.at[dst_at],
            send_sem=sum_sems.at[send],
            recv_sem=sum_sems.at[recv],
            device_id=device,
            device_id_type=MESH,
        ).start()

    sum_gy[gy] = mine
    for p in gy_peers:
        send_row(sum_gy, gy, sum_gy, gy, 0, 1, (gx, p))
    rows_of(sum_gy, ngy - 1, sum_sems.at[1]).wait()
    total = sum_gy[0]
    for k in range(1, ngy):
        total = total + sum_gy[k]

    sum_plane[gx] = total
    for hub in hubs:

        @pl.when(gx != hub)
        def _():
            send_row(sum_plane, gx, sum_plane, gx, 2, 3, (hub, gy))

    @pl.when(is_hub)
    def _():
        rows_of(sum_plane, ngx - 1, sum_sems.at[3]).wait()
        whole = sum_plane[0]
        for k in range(1, ngx):
            whole = whole + sum_plane[k]
        result[0] = whole
        result[1] = whole
        for z in later:

            @pl.when(zz == nhub - 1)
            def _():
                send_row(result, 0, result, 1, 4, 5, (yy * nz + z, gy))

    @pl.when(jnp.logical_not(is_hub))
    def _():
        rows_of(result, 1, sum_sems.at[5]).wait()

    total = result[1]

    def item(k):
        return total[0:1, k : k + 1]

    def solve(k11, k12, k22, k1, k2):
        scale = 1.0 / item(k11)
        a12, a22 = item(k12) * scale, item(k22) * scale
        f1, f2 = item(k1) * scale, item(k2) * scale
        det = 1.0 / (a22 - a12 * a12)
        return (a22 * f1 - a12 * f2) * det, (f2 - a12 * f1) * det

    c1, c2 = solve(0, 1, 2, 3, 4)
    d1, d2 = solve(5, 6, 7, 8, 9)
    velocity[0] = v_guess[0] + c1 * local[0] + c2 * local[3]
    velocity[1] = v_guess[1] + c1 * local[1] + c2 * local[4]
    level[...] = v_oguess[...] + d1 * local[2] + d2 * local[5]

    for k in range(3):

        @pl.when(jnp.logical_and(top, jnp.logical_not(mirror_self[k])))
        def _():
            fold[k].wait_send()

    for at, served in posts.items():

        @pl.when(jnp.logical_and(top, zz == at))
        def _():
            for slot, _ in enumerate(served):
                pltpu.make_async_copy(post_in.at[slot], post_in.at[slot], post_send.at[slot]).wait()

    @pl.when(jnp.logical_not(top))
    def _():
        for copy in up:
            copy.wait_send()

    @pl.when(jnp.logical_not(bottom))
    def _():
        for k in range(3):
            down[k].wait_send()

    to_east.wait_send()
    to_west.wait_send()
    rows_of(sum_gy, ngy - 1, sum_sems.at[0]).wait()

    @pl.when(is_hub)
    def _():
        rows_of(sum_plane, len(hubs) - 1, sum_sems.at[2]).wait()

    @pl.when(jnp.logical_not(is_hub))
    def _():
        rows_of(sum_plane, len(hubs), sum_sems.at[2]).wait()

    @pl.when(zz == nhub - 1)
    def _():
        rows_of(sum_plane, len(later), sum_sems.at[4]).wait()


def put_out(velocity, level, velocity_out, level_out, sems):
    copies = [
        pltpu.make_async_copy(velocity, velocity_out, sems.at[0]),
        pltpu.make_async_copy(level, level_out, sems.at[1]),
    ]
    for copy in copies:
        copy.start()
    for copy in copies:
        copy.wait()


def build(mesh, ny, nz, interpret=False):
    ngy = mesh.shape["gy"]
    f32 = jnp.float32
    block = pltpu.VMEM((ROWS, COLS), f32)
    pair = pltpu.VMEM((2, ROWS, COLS), f32)
    whole = pltpu.VMEM((ROWS, COLS), jnp.int32)
    dma = pltpu.SemaphoreType.DMA

    def body(*args):
        solved = pl.pallas_call(
            functools.partial(kernel, (ny, nz, ngy)),
            out_shape=(
                pltpu.VMEM((2, ROWS, COLS), f32),
                pltpu.VMEM((ROWS, COLS), f32),
            ),
            in_specs=[pl.BlockSpec(memory_space=pl.ANY)] * 10,
            out_specs=(pl.BlockSpec(memory_space=pltpu.VMEM), pl.BlockSpec(memory_space=pltpu.VMEM)),
            scratch_shapes=[
                pair,
                pair,
                block,
                block,
                block,
                block,
                block,
                block,
                whole,
                whole,
                pltpu.VMEM((9, EXT_ROWS, EXT_COLS), f32),
                pltpu.VMEM((7, ROWS, COLS), f32),
                pltpu.VMEM((2, 3, 8, COLS), f32),
                pltpu.VMEM((2, 3, 8, COLS), f32),
                pltpu.VMEM((2, PACK, 128), f32),
                pltpu.VMEM((2, 8, 128), f32),
                pltpu.VMEM((STRIP, 128), f32),
                pltpu.VMEM((STRIP, 128), f32),
                pltpu.VMEM((nz - 2 * nz // 3, STRIP, 128), f32),
                pltpu.VMEM((ngy, 1, 128), f32),
                pltpu.VMEM((ny * nz, 1, 128), f32),
                pltpu.VMEM((2, 1, 128), f32),
                dma((10,)),
                dma((8,)),
                dma((8,)),
                dma((nz - 2 * nz // 3,)),
                dma((nz - 2 * nz // 3,)),
                dma((6,)),
            ],
            compiler_params=pltpu.CompilerParams(collective_id=0, has_side_effects=True, vmem_limit_bytes=16 * 1024 * 1024),
            name="picard",
        )(*[pltpu.with_memory_space_constraint(a, pltpu.HBM) for a in args])
        return pl.pallas_call(
            put_out,
            out_shape=(pltpu.HBM((2, ROWS, COLS), f32), pltpu.HBM((ROWS, COLS), f32)),
            in_specs=[pl.BlockSpec(memory_space=pltpu.VMEM)] * 2,
            out_specs=(pl.BlockSpec(memory_space=pltpu.HBM), pl.BlockSpec(memory_space=pltpu.HBM)),
            scratch_shapes=[dma((2,))],
            compiler_params=pltpu.CompilerParams(vmem_limit_bytes=4 * 1024 * 1024),
            name="put_out",
        )(*[pltpu.with_memory_space_constraint(a, pltpu.VMEM) for a in solved])

    both = P(None, "gx", "gy")
    one = P("gx", "gy")
    return jax.shard_map(
        body,
        mesh=mesh,
        in_specs=(both, both, one, one, one, one, one, one, one, one),
        out_specs=(both, one),
        check_vma=False,
    )


def solution(mesh):
    return build(mesh, 8, 12)
```

```python
import functools

import jax
import jax.numpy as jnp
from jax import lax
from jax.experimental import pallas as pl
from jax.experimental.pallas import tpu as pltpu
from jax.sharding import PartitionSpec as P

MESH = pl.DeviceIdType.MESH

M_U, M_V, H_U, H_V, M_O, H_O, B_I, B_O, TURN = range(9)
DEPTH = {M_U: 3, M_V: 3, M_O: 3, H_U: 2, H_V: 2, H_O: 2, B_I: 2, B_O: 2, TURN: 1}
HALVES = ((M_U, M_V, H_U, H_V), (M_O, H_O, B_I, B_O, TURN))
TILES = ((M_U, M_V, H_U), (M_O, H_V, H_O, TURN), (B_I, B_O))
PACK = 24
STRIP = PACK + 16
HUBS = 4
ROWS = 64
COLS = 256
EXT_ROWS = ROWS + 8
EXT_COLS = COLS + 128


def iota(shape, dim):
    return lax.broadcasted_iota(jnp.int32, shape, dim)


def roll(x, by, dim):
    size = x.shape[dim]
    return x if by % size == 0 else pltpu.roll(x, by % size, dim)


def columns():
    for half, fields in enumerate(HALVES):
        at = 0
        for f in fields:
            yield half, f, at, DEPTH[f]
            at += 2 * DEPTH[f]


def packed_rows():
    for t, fields in enumerate(TILES):
        at = 0
        for f in fields:
            yield t, f, at, DEPTH[f]
            at += DEPTH[f]


def northern_rows():
    row, lane = iota((PACK, 128), 0), iota((PACK, 128), 1)
    step = jnp.full((PACK, 128), -1, jnp.int32)
    for half, _, at, n in columns():
        here = (lane < 64) if half == 0 else (lane >= 64)
        for k in range(n):
            step = jnp.where(jnp.logical_and(here, row == at + n + k), k, step)
    return step


def corners(turned):
    lane = lax.rem(iota((8, 128), 1) + 2, 64)
    first, second, third = [roll(turned[8 * t : 8 * t + 8], 4 * t, 1) for t in range(3)]
    return jnp.where(lane < 4, first, jnp.where(lane < 8, second, third))


def from_corners(tile):
    return jnp.concatenate([roll(tile, -4 * t, 1) for t in range(3)], axis=0)


def around(q):
    rows, cols = q.shape
    return (
        pltpu.roll(q, 1, 0) + pltpu.roll(q, rows - 1, 0) + pltpu.roll(q, 1, 1) + pltpu.roll(q, cols - 1, 1)
    )


def inner_block(x):
    return x[:ROWS, :COLS]


def kernel(
    sizes,
    ice_rhs,
    ice_guess,
    ocean_rhs,
    ocean_guess,
    ice_diag,
    ice_visc,
    coriolis,
    depth_factor,
    wet_mask,
    ice_mask,
    velocity,
    level,
    v_rhs,
    v_guess,
    v_orhs,
    v_oguess,
    v_diag,
    v_visc,
    v_cor,
    v_depth,
    v_wet,
    v_ice,
    fields,
    local,
    zonal_out,
    zonal_in,
    merid_out,
    corner_out,
    north_in,
    south_in,
    post_in,
    sum_gy,
    sum_plane,
    result,
    load_sems,
    halo_send,
    halo_recv,
    post_send,
    post_recv,
    sum_sems,
):
    ny, nz, ngy = sizes
    ngx = ny * nz
    gx = lax.axis_index("gx")
    gy = lax.axis_index("gy")
    yy = gx // nz
    zz = lax.rem(gx, nz)
    top = gy == ngy - 1
    bottom = gy == 0

    loads = []
    for i, (src, dst) in enumerate(
        (
            (ice_rhs, v_rhs),
            (ice_guess, v_guess),
            (ocean_rhs, v_orhs),
            (ocean_guess, v_oguess),
            (ice_diag, v_diag),
            (ice_visc, v_visc),
            (coriolis, v_cor),
            (depth_factor, v_depth),
            (wet_mask, v_wet),
            (ice_mask, v_ice),
        )
    ):
        loads.append(pltpu.make_async_copy(src, dst, load_sems.at[i]))

    def wrap(x):
        return lax.rem(x + ngx, ngx)

    def north_of(step):
        there = wrap(gx + step)
        return jnp.where(top, ngx - 1 - there, there), jnp.where(top, gy, gy + 1)

    def south_of(step):
        return wrap(gx + step), jnp.where(bottom, gy, gy - 1)

    east = (wrap(gx + 1), gy)
    west = (wrap(gx - 1), gy)
    norths = [north_of(step) for step in (0, 1, -1)]
    souths = [south_of(step) for step in (0, 1, -1)]
    gy_peers = [lax.rem(gy + d, ngy) for d in range(1, ngy)]
    nhub = min(HUBS, nz - 1)
    hubs = [y * nz + z for z in range(nhub) for y in range(ny)]
    is_hub = zz < nhub
    later = [z for z in range(nhub, nz)]

    barrier = pltpu.get_barrier_semaphore()

    def greet(device):
        pl.semaphore_signal(barrier, inc=1, device_id=device, device_id_type=MESH)

    far_z = 2 * nz // 3
    posts = {}
    for z in range(nz // 2, nz):
        posts.setdefault(0 if z >= far_z else nz - 1 - z, []).append(z)

    def is_late(g):
        return 2 * lax.rem(g, nz) >= nz

    def post_of(g):
        z = lax.rem(g, nz)
        far = z >= far_z
        return g - z + jnp.where(far, 0, nz - 1 - z), jnp.where(far, z - far_z, 0)

    def mirrors(g):
        return [ngx - 1 - wrap(g + step) for step in (0, 1, -1)]

    late = is_late(gx)
    mirror_self = [
        jnp.logical_and(jnp.logical_and(top, jnp.logical_not(late)), norths[k][0] == gx) for k in range(3)
    ]

    for copy in loads:
        copy.start()

    @pl.when(is_hub)
    def _():
        for z in sorted(range(nz), key=lambda z: abs(z - nz // 3)):
            for d in sorted(range(ny), key=lambda d: -min(d, ny - d)):
                there = (lax.rem(yy + d, ny) * nz + z, gy)
                if d == 0 and z < nhub:

                    @pl.when(zz != z)
                    def _():
                        greet(there)

                else:
                    greet(there)

    @pl.when(jnp.logical_and(top, late))
    def _():
        greet((post_of(gx)[0], gy))

    for k in range(3):

        @pl.when(jnp.logical_not(jnp.logical_or(jnp.logical_and(top, late), mirror_self[k])))
        def _():
            greet(norths[k])

    greet(east)
    greet(west)
    for p in gy_peers:
        greet((gx, p))

    @pl.when(jnp.logical_not(bottom))
    def _():
        for device in souths:
            greet(device)

    for at, served in posts.items():

        @pl.when(jnp.logical_and(top, zz == at))
        def _():
            for z in served:
                for g in mirrors(yy * nz + z):
                    greet((g, gy))

    for copy in loads:
        copy.wait()

    wet = v_wet[...].astype(jnp.float32)
    active = wet * v_ice[...].astype(jnp.float32)
    visc = v_visc[...]
    depth = v_depth[...]
    d_i = active * (v_diag[...] + 4.0 * visc * visc) + 1.0 - active
    d_o = wet * (1.0 + 4.0 * depth * depth) + 1.0 - wet
    p_i = 1.0 / d_i
    p_o = 1.0 / d_o
    r_i = active * visc
    r_o = wet * depth
    s_i = r_i * p_i
    s_o = r_o * p_o
    c = active * v_cor[...]
    g_u = v_guess[0]
    g_v = v_guess[1]
    g_o = v_oguess[...]
    h_u = v_rhs[0] - d_i * g_u + c * g_v
    h_v = v_rhs[1] - d_i * g_v - c * g_u
    h_o = v_orhs[...] - d_o * g_o
    own = {
        M_U: r_i * g_u,
        M_V: r_i * g_v,
        M_O: r_o * g_o,
        H_U: s_i * h_u,
        H_V: s_i * h_v,
        H_O: s_o * h_o,
        B_I: r_i * s_i,
        B_O: r_o * s_o,
        TURN: c * p_i,
    }
    for k, value in enumerate((h_u, h_v, h_o, r_i, r_o, p_i, p_o)):
        local[k] = value
    for f in range(9):
        fields[f, 0:ROWS, 0:COLS] = own[f]

    sub = iota((8, COLS), 0)
    eastward = [jnp.zeros((8, COLS), jnp.float32)] * len(TILES)
    westward = [jnp.zeros((8, COLS), jnp.float32)] * len(TILES)
    for t, f, at, n in packed_rows():
        eastward[t] = jnp.where(
            jnp.logical_and(sub >= 8 - at - n, sub < 8 - at), roll(own[f][ROWS - 8 : ROWS], -at, 0), eastward[t]
        )
        westward[t] = jnp.where(jnp.logical_and(sub >= at, sub < at + n), roll(own[f][0:8], at, 0), westward[t])
    for t in range(len(TILES)):
        zonal_out[0, t] = eastward[t]
        zonal_out[1, t] = westward[t]

    lane = iota((ROWS, 128), 1)
    halves = [jnp.zeros((ROWS, 128), jnp.float32)] * 2
    for half, f, at, n in columns():
        edge = jnp.where(lane < 64, own[f][:, 0:128], own[f][:, COLS - 128 : COLS])
        halves[half] = jnp.where(
            jnp.logical_and(lane >= at, lane < at + 2 * n), roll(edge, at + n, 1), halves[half]
        )
    turned = jnp.transpose(jnp.concatenate(halves, axis=0))[0:PACK]
    merid_out[0] = turned
    merid_out[1] = turned
    corner_out[0] = corners(turned)
    corner_out[1] = corners(turned)

    @pl.when(top)
    def _():
        step = northern_rows()
        flipped = jnp.where(
            step == 0, roll(turned, 1, 0), jnp.where(step == 1, roll(turned, 3, 0), roll(turned, 5, 0))
        )
        swap = jnp.where(
            (iota((128, 128), 0) ^ iota((128, 128), 1)) == 63, 1.0, 0.0
        ).astype(jnp.float32)
        mirrored = jnp.dot(
            flipped, swap, precision=lax.Precision.HIGHEST, preferred_element_type=jnp.float32
        )
        mirrored = jnp.where(iota((PACK, 128), 1) < 64, -mirrored, mirrored)
        merid_out[0] = mirrored
        corner_out[0] = corners(mirrored)

    @pl.when(bottom)
    def _():
        south_in[...] = jnp.zeros((STRIP, 128), jnp.float32)

    expected = len(hubs) + ngy - 1 + 2 + 3 + jnp.where(bottom, 0, 3) - jnp.where(is_hub, 1, 0)
    for k in range(3):
        expected = expected - jnp.where(mirror_self[k], 1, 0)
    for at, served in posts.items():
        expected = expected + jnp.where(jnp.logical_and(top, zz == at), len(served), 0)
    pl.semaphore_wait(barrier, expected)

    def remote(src, dst, sent, got, device):
        return pltpu.make_async_remote_copy(
            src_ref=src,
            dst_ref=dst,
            send_sem=halo_send.at[sent],
            recv_sem=halo_recv.at[got],
            device_id=device,
            device_id_type=MESH,
        )

    parts = [pl.ds(0, PACK), pl.ds(PACK, 8), pl.ds(PACK + 8, 8)]
    opposite = (0, 2, 1)
    sources = [[merid_out.at[i], corner_out.at[i], corner_out.at[i]] for i in range(2)]
    fold = [remote(sources[0][k], north_in.at[parts[k]], k, k, norths[k]) for k in range(3)]
    up = [
        remote(sources[0][k], south_in.at[parts[opposite[k]]], k, 3 + opposite[k], norths[k])
        for k in range(3)
    ]
    down = [
        remote(sources[1][k], north_in.at[parts[opposite[k]]], 3 + k, opposite[k], souths[k])
        for k in range(3)
    ]

    def to_post(k):
        post, slot = post_of(norths[k][0])
        return pltpu.make_async_remote_copy(
            src_ref=sources[0][k],
            dst_ref=post_in.at[slot, parts[k]],
            send_sem=halo_send.at[k],
            recv_sem=post_recv.at[slot],
            device_id=(post, gy),
            device_id_type=MESH,
        )

    to_east = remote(zonal_out.at[0], zonal_in.at[0], 6, 6, east)
    to_west = remote(zonal_out.at[1], zonal_in.at[1], 7, 7, west)

    target_late = [is_late(norths[k][0]) for k in range(3)]
    for k in range(3):

        @pl.when(jnp.logical_and(top, target_late[k]))
        def _():
            to_post(k).start()

        @pl.when(
            jnp.logical_and(
                jnp.logical_and(top, jnp.logical_not(target_late[k])), jnp.logical_not(mirror_self[k])
            )
        )
        def _():
            fold[k].start()

        @pl.when(mirror_self[k])
        def _():
            north_in[PACK + 8 * max(k - 1, 0) : PACK + 8 * max(k - 1, 0) + 8] = corner_out[0]

    @pl.when(jnp.logical_not(top))
    def _():
        for copy in up:
            copy.start()

    @pl.when(jnp.logical_not(bottom))
    def _():
        for copy in down:
            copy.start()

    to_east.start()
    to_west.start()

    for at, served in posts.items():

        @pl.when(jnp.logical_and(top, zz == at))
        def _():
            for slot, z in enumerate(served):
                strip = post_in.at[slot]
                pltpu.make_async_copy(strip, strip, post_recv.at[slot]).wait()
                pltpu.make_async_remote_copy(
                    src_ref=strip,
                    dst_ref=north_in,
                    send_sem=post_send.at[slot],
                    recv_sem=halo_recv.at[0],
                    device_id=(yy * nz + z, gy),
                    device_id_type=MESH,
                ).start()

    to_east.wait_recv()
    to_west.wait_recv()

    for t, f, at, n in packed_rows():
        fields[f, ROWS:EXT_ROWS, 0:COLS] = jnp.where(
            sub < 4, roll(zonal_in[1, t], -at, 0), roll(zonal_in[0, t], at, 0)
        )

    def arrived(k, dst):
        pltpu.make_async_copy(dst, dst, halo_recv.at[k]).wait()

    @pl.when(jnp.logical_and(top, late))
    def _():
        arrived(0, north_in)

    for k in range(3):

        @pl.when(jnp.logical_not(jnp.logical_or(jnp.logical_and(top, late), mirror_self[k])))
        def _():
            arrived(k, north_in.at[parts[k]])

        @pl.when(jnp.logical_not(bottom))
        def _():
            arrived(3 + k, south_in.at[parts[k]])

    northern = northern_rows() >= 0
    plane = jnp.where(northern, north_in[0:PACK], south_in[0:PACK])
    from_e, from_w = [
        jnp.where(northern, from_corners(north_in[at : at + 8]), from_corners(south_in[at : at + 8]))
        for at in (PACK, PACK + 8)
    ]
    lane = iota((PACK, 128), 1)
    pad = jnp.zeros((128 - PACK, 128), jnp.float32)
    backs = []
    for half in range(2):
        if half == 0:
            center, right, left = plane, roll(from_e, 64, 1), roll(from_w, 8, 1)
        else:
            center, right, left = roll(plane, 64, 1), from_e, roll(from_w, 72, 1)
        merged = jnp.where(lane < 64, center, jnp.where(lane < 68, right, left))
        backs.append(jnp.transpose(jnp.concatenate([merged, pad], axis=0))[0:EXT_ROWS])
    for half, f, at, n in columns():
        fields[f, :, COLS:EXT_COLS] = roll(backs[half], -(at + n), 1)

    b_i = fields[B_I]
    b_o = fields[B_O]
    turn = fields[TURN]
    t_in = inner_block(turn)
    h_u, h_v, h_o = local[0], local[1], local[2]
    r_i, r_o, p_i, p_o = local[3], local[4], local[5], local[6]
    nb_u = around(fields[M_U])
    nb_v = around(fields[M_V])
    nb_o = around(fields[M_O])
    s0_u = fields[H_U] + b_i * nb_u
    s0_v = fields[H_V] + b_i * nb_v
    s0_o = fields[H_O] + b_o * nb_o
    res_u = h_u + r_i * inner_block(nb_u)
    res_v = h_v + r_i * inner_block(nb_v)
    res_o = h_o + r_o * inner_block(nb_o)
    nb_u = around(s0_u)
    nb_v = around(s0_v)
    nb_o = around(s0_o)
    s1_u = b_i * nb_u + turn * s0_v
    s1_v = b_i * nb_v - turn * s0_u
    s1_o = b_o * nb_o
    n1_u = r_i * inner_block(nb_u) + t_in * res_v
    n1_v = r_i * inner_block(nb_v) - t_in * res_u
    n1_o = r_o * inner_block(nb_o)
    n2_u = r_i * inner_block(around(s1_u)) + t_in * n1_v
    n2_v = r_i * inner_block(around(s1_v)) - t_in * n1_u
    n2_o = r_o * inner_block(around(s1_o))
    a_u, a_v, a_o = res_u - n1_u, res_v - n1_v, res_o - n1_o
    e_u, e_v, e_o = n1_u - n2_u, n1_v - n2_v, n1_o - n2_o
    z_o = p_o * res_o
    x_o = p_o * n1_o
    products = [
        a_u * a_u + a_v * a_v,
        a_u * e_u + a_v * e_v,
        e_u * e_u + e_v * e_v,
        a_u * res_u + a_v * res_v,
        e_u * res_u + e_v * res_v,
        z_o * a_o,
        x_o * a_o,
        x_o * e_o,
        z_o * res_o,
        x_o * res_o,
    ]
    local[0] = p_i * res_u
    local[1] = p_i * res_v
    local[2] = z_o
    local[3] = p_i * n1_u
    local[4] = p_i * n1_v
    local[5] = x_o

    row = iota((16, 128), 0)
    sums = jnp.zeros((16, 128), jnp.float32)
    for k, product in enumerate(products):
        half = product[:, 0:128] + product[:, 128:256]
        sums = jnp.where(row == k, jnp.sum(half, axis=0, keepdims=True), sums)
    sums = jnp.sum(sums, axis=1, keepdims=True)
    mine = jnp.sum(jnp.where(row == iota((16, 128), 1), sums, 0.0), axis=0, keepdims=True)

    def rows_of(slots, count, sem):
        return pltpu.make_async_copy(slots.at[pl.ds(0, count)], slots.at[pl.ds(0, count)], sem)

    def send_row(slots, at, dst, dst_at, send, recv, device):
        pltpu.make_async_remote_copy(
            src_ref=slots.at[at],
            dst_ref=dst.at[dst_at],
            send_sem=sum_sems.at[send],
            recv_sem=sum_sems.at[recv],
            device_id=device,
            device_id_type=MESH,
        ).start()

    sum_gy[gy] = mine
    for p in gy_peers:
        send_row(sum_gy, gy, sum_gy, gy, 0, 1, (gx, p))
    rows_of(sum_gy, ngy - 1, sum_sems.at[1]).wait()
    total = sum_gy[0]
    for k in range(1, ngy):
        total = total + sum_gy[k]

    sum_plane[gx] = total
    for hub in hubs:

        @pl.when(gx != hub)
        def _():
            send_row(sum_plane, gx, sum_plane, gx, 2, 3, (hub, gy))

    @pl.when(is_hub)
    def _():
        rows_of(sum_plane, ngx - 1, sum_sems.at[3]).wait()
        parts_of = [sum_plane[k] for k in range(8)]
        for k in range(8, ngx):
            parts_of[k % 8] = parts_of[k % 8] + sum_plane[k]
        while len(parts_of) > 1:
            parts_of = [a + b for a, b in zip(parts_of[0::2], parts_of[1::2])]
        whole = parts_of[0]
        result[0] = whole
        result[1] = whole
        for z in later:

            @pl.when(zz == nhub - 1)
            def _():
                send_row(result, 0, result, 1, 4, 5, (yy * nz + z, gy))

    @pl.when(jnp.logical_not(is_hub))
    def _():
        rows_of(result, 1, sum_sems.at[5]).wait()

    total = result[1]

    def item(k):
        return total[0:1, k : k + 1]

    def solve(k11, k12, k22, k1, k2):
        scale = 1.0 / item(k11)
        a12, a22 = item(k12) * scale, item(k22) * scale
        f1, f2 = item(k1) * scale, item(k2) * scale
        det = 1.0 / (a22 - a12 * a12)
        return (a22 * f1 - a12 * f2) * det, (f2 - a12 * f1) * det

    c1, c2 = solve(0, 1, 2, 3, 4)
    d1, d2 = solve(5, 6, 7, 8, 9)
    velocity[0] = v_guess[0] + c1 * local[0] + c2 * local[3]
    velocity[1] = v_guess[1] + c1 * local[1] + c2 * local[4]
    level[...] = v_oguess[...] + d1 * local[2] + d2 * local[5]

    for k in range(3):

        @pl.when(jnp.logical_and(top, jnp.logical_not(mirror_self[k])))
        def _():
            fold[k].wait_send()

    for at, served in posts.items():

        @pl.when(jnp.logical_and(top, zz == at))
        def _():
            for slot, _ in enumerate(served):
                pltpu.make_async_copy(post_in.at[slot], post_in.at[slot], post_send.at[slot]).wait()

    @pl.when(jnp.logical_not(top))
    def _():
        for copy in up:
            copy.wait_send()

    @pl.when(jnp.logical_not(bottom))
    def _():
        for k in range(3):
            down[k].wait_send()

    to_east.wait_send()
    to_west.wait_send()
    rows_of(sum_gy, ngy - 1, sum_sems.at[0]).wait()

    @pl.when(is_hub)
    def _():
        rows_of(sum_plane, len(hubs) - 1, sum_sems.at[2]).wait()

    @pl.when(jnp.logical_not(is_hub))
    def _():
        rows_of(sum_plane, len(hubs), sum_sems.at[2]).wait()

    @pl.when(zz == nhub - 1)
    def _():
        rows_of(sum_plane, len(later), sum_sems.at[4]).wait()


def put_out(velocity, level, velocity_out, level_out, sems):
    copies = [
        pltpu.make_async_copy(velocity, velocity_out, sems.at[0]),
        pltpu.make_async_copy(level, level_out, sems.at[1]),
    ]
    for copy in copies:
        copy.start()
    for copy in copies:
        copy.wait()


def build(mesh, ny, nz, interpret=False):
    ngy = mesh.shape["gy"]
    f32 = jnp.float32
    block = pltpu.VMEM((ROWS, COLS), f32)
    pair = pltpu.VMEM((2, ROWS, COLS), f32)
    whole = pltpu.VMEM((ROWS, COLS), jnp.int32)
    dma = pltpu.SemaphoreType.DMA

    def body(*args):
        solved = pl.pallas_call(
            functools.partial(kernel, (ny, nz, ngy)),
            out_shape=(
                pltpu.VMEM((2, ROWS, COLS), f32),
                pltpu.VMEM((ROWS, COLS), f32),
            ),
            in_specs=[pl.BlockSpec(memory_space=pl.ANY)] * 10,
            out_specs=(pl.BlockSpec(memory_space=pltpu.VMEM), pl.BlockSpec(memory_space=pltpu.VMEM)),
            scratch_shapes=[
                pair,
                pair,
                block,
                block,
                block,
                block,
                block,
                block,
                whole,
                whole,
                pltpu.VMEM((9, EXT_ROWS, EXT_COLS), f32),
                pltpu.VMEM((7, ROWS, COLS), f32),
                pltpu.VMEM((2, 3, 8, COLS), f32),
                pltpu.VMEM((2, 3, 8, COLS), f32),
                pltpu.VMEM((2, PACK, 128), f32),
                pltpu.VMEM((2, 8, 128), f32),
                pltpu.VMEM((STRIP, 128), f32),
                pltpu.VMEM((STRIP, 128), f32),
                pltpu.VMEM((nz - 2 * nz // 3, STRIP, 128), f32),
                pltpu.VMEM((ngy, 1, 128), f32),
                pltpu.VMEM((ny * nz, 1, 128), f32),
                pltpu.VMEM((2, 1, 128), f32),
                dma((10,)),
                dma((8,)),
                dma((8,)),
                dma((nz - 2 * nz // 3,)),
                dma((nz - 2 * nz // 3,)),
                dma((6,)),
            ],
            compiler_params=pltpu.CompilerParams(collective_id=0, has_side_effects=True, vmem_limit_bytes=16 * 1024 * 1024),
            name="picard",
        )(*[pltpu.with_memory_space_constraint(a, pltpu.HBM) for a in args])
        return pl.pallas_call(
            put_out,
            out_shape=(pltpu.HBM((2, ROWS, COLS), f32), pltpu.HBM((ROWS, COLS), f32)),
            in_specs=[pl.BlockSpec(memory_space=pltpu.VMEM)] * 2,
            out_specs=(pl.BlockSpec(memory_space=pltpu.HBM), pl.BlockSpec(memory_space=pltpu.HBM)),
            scratch_shapes=[dma((2,))],
            compiler_params=pltpu.CompilerParams(vmem_limit_bytes=4 * 1024 * 1024),
            name="put_out",
        )(*[pltpu.with_memory_space_constraint(a, pltpu.VMEM) for a in solved])

    both = P(None, "gx", "gy")
    one = P("gx", "gy")
    return jax.shard_map(
        body,
        mesh=mesh,
        in_specs=(both, both, one, one, one, one, one, one, one, one),
        out_specs=(both, one),
        check_vma=False,
    )


def solution(mesh):
    return build(mesh, 8, 12)
```

```python
import functools

import jax
import jax.numpy as jnp
from jax import lax
from jax.experimental import pallas as pl
from jax.experimental.pallas import tpu as pltpu
from jax.sharding import PartitionSpec as P

MESH = pl.DeviceIdType.MESH

M_U, M_V, H_U, H_V, M_O, H_O, B_I, B_O, TURN = range(9)
DEPTH = {M_U: 3, M_V: 3, M_O: 3, H_U: 2, H_V: 2, H_O: 2, B_I: 2, B_O: 2, TURN: 1}
HALVES = ((M_U, M_V, H_U, H_V), (M_O, H_O, B_I, B_O, TURN))
TILES = ((M_U, M_V, H_U), (M_O, H_V, H_O, TURN), (B_I, B_O))
PACK = 24
STRIP = PACK + 16
HUBS = 4
ROWS = 64
COLS = 256
EXT_ROWS = ROWS + 8
EXT_COLS = COLS + 128


def iota(shape, dim):
    return lax.broadcasted_iota(jnp.int32, shape, dim)


def roll(x, by, dim):
    size = x.shape[dim]
    return x if by % size == 0 else pltpu.roll(x, by % size, dim)


def columns():
    for half, fields in enumerate(HALVES):
        at = 0
        for f in fields:
            yield half, f, at, DEPTH[f]
            at += 2 * DEPTH[f]


def packed_rows():
    for t, fields in enumerate(TILES):
        at = 0
        for f in fields:
            yield t, f, at, DEPTH[f]
            at += DEPTH[f]


def northern_rows():
    row, lane = iota((PACK, 128), 0), iota((PACK, 128), 1)
    step = jnp.full((PACK, 128), -1, jnp.int32)
    for half, _, at, n in columns():
        here = (lane < 64) if half == 0 else (lane >= 64)
        for k in range(n):
            step = jnp.where(jnp.logical_and(here, row == at + n + k), k, step)
    return step


def corners(turned):
    lane = lax.rem(iota((8, 128), 1) + 2, 64)
    first, second, third = [roll(turned[8 * t : 8 * t + 8], 4 * t, 1) for t in range(3)]
    return jnp.where(lane < 4, first, jnp.where(lane < 8, second, third))


def from_corners(tile):
    return jnp.concatenate([roll(tile, -4 * t, 1) for t in range(3)], axis=0)


def around(q):
    rows, cols = q.shape
    return (
        pltpu.roll(q, 1, 0) + pltpu.roll(q, rows - 1, 0) + pltpu.roll(q, 1, 1) + pltpu.roll(q, cols - 1, 1)
    )


def inner_block(x):
    return x[:ROWS, :COLS]


def kernel(
    sizes,
    ice_rhs,
    ice_guess,
    ocean_rhs,
    ocean_guess,
    ice_diag,
    ice_visc,
    coriolis,
    depth_factor,
    wet_mask,
    ice_mask,
    velocity,
    level,
    v_rhs,
    v_guess,
    v_orhs,
    v_oguess,
    v_diag,
    v_visc,
    v_cor,
    v_depth,
    v_wet,
    v_ice,
    fields,
    local,
    zonal_out,
    zonal_in,
    merid_out,
    corner_out,
    north_in,
    south_in,
    post_in,
    sum_gy,
    sum_plane,
    result,
    load_sems,
    halo_send,
    halo_recv,
    post_send,
    post_recv,
    sum_sems,
):
    ny, nz, ngy = sizes
    ngx = ny * nz
    gx = lax.axis_index("gx")
    gy = lax.axis_index("gy")
    yy = gx // nz
    zz = lax.rem(gx, nz)
    top = gy == ngy - 1
    bottom = gy == 0

    loads = []
    for i, (src, dst) in enumerate(
        (
            (ice_rhs, v_rhs),
            (ice_guess, v_guess),
            (ocean_rhs, v_orhs),
            (ocean_guess, v_oguess),
            (ice_diag, v_diag),
            (ice_visc, v_visc),
            (coriolis, v_cor),
            (depth_factor, v_depth),
            (wet_mask, v_wet),
            (ice_mask, v_ice),
        )
    ):
        loads.append(pltpu.make_async_copy(src, dst, load_sems.at[i]))

    def wrap(x):
        return lax.rem(x + ngx, ngx)

    def north_of(step):
        there = wrap(gx + step)
        return jnp.where(top, ngx - 1 - there, there), jnp.where(top, gy, gy + 1)

    def south_of(step):
        return wrap(gx + step), jnp.where(bottom, gy, gy - 1)

    east = (wrap(gx + 1), gy)
    west = (wrap(gx - 1), gy)
    norths = [north_of(step) for step in (0, 1, -1)]
    souths = [south_of(step) for step in (0, 1, -1)]
    gy_peers = [lax.rem(gy + d, ngy) for d in range(1, ngy)]
    nhub = min(HUBS, nz - 1)
    hubs = [y * nz + z for z in range(nhub) for y in range(ny)]
    is_hub = zz < nhub
    later = [z for z in range(nhub, nz)]

    barrier = pltpu.get_barrier_semaphore()

    def greet(device):
        pl.semaphore_signal(barrier, inc=1, device_id=device, device_id_type=MESH)

    far_z = 2 * nz // 3
    posts = {}
    for z in range(nz // 2, nz):
        posts.setdefault(0 if z >= far_z else nz - 1 - z, []).append(z)

    def is_late(g):
        return 2 * lax.rem(g, nz) >= nz

    def post_of(g):
        z = lax.rem(g, nz)
        far = z >= far_z
        return g - z + jnp.where(far, 0, nz - 1 - z), jnp.where(far, z - far_z, 0)

    def mirrors(g):
        return [ngx - 1 - wrap(g + step) for step in (0, 1, -1)]

    late = is_late(gx)
    mirror_self = [
        jnp.logical_and(jnp.logical_and(top, jnp.logical_not(late)), norths[k][0] == gx) for k in range(3)
    ]

    for copy in loads:
        copy.start()

    @pl.when(is_hub)
    def _():
        for z in sorted(range(nz), key=lambda z: abs(z - nz // 3)):
            for d in sorted(range(ny), key=lambda d: -min(d, ny - d)):
                there = (lax.rem(yy + d, ny) * nz + z, gy)
                if d == 0 and z < nhub:

                    @pl.when(zz != z)
                    def _():
                        greet(there)

                else:
                    greet(there)

    @pl.when(jnp.logical_and(top, late))
    def _():
        greet((post_of(gx)[0], gy))

    for k in range(3):

        @pl.when(jnp.logical_not(jnp.logical_or(jnp.logical_and(top, late), mirror_self[k])))
        def _():
            greet(norths[k])

    greet(east)
    greet(west)
    for p in gy_peers:
        greet((gx, p))

    @pl.when(jnp.logical_not(bottom))
    def _():
        for device in souths:
            greet(device)

    for at, served in posts.items():

        @pl.when(jnp.logical_and(top, zz == at))
        def _():
            for z in served:
                for g in mirrors(yy * nz + z):
                    greet((g, gy))

    for copy in loads:
        copy.wait()

    wet = v_wet[...].astype(jnp.float32)
    active = wet * v_ice[...].astype(jnp.float32)
    visc = v_visc[...]
    depth = v_depth[...]
    d_i = active * (v_diag[...] + 4.0 * visc * visc) + 1.0 - active
    d_o = wet * (1.0 + 4.0 * depth * depth) + 1.0 - wet
    p_i = 1.0 / d_i
    p_o = 1.0 / d_o
    r_i = active * visc
    r_o = wet * depth
    s_i = r_i * p_i
    s_o = r_o * p_o
    c = active * v_cor[...]
    g_u = v_guess[0]
    g_v = v_guess[1]
    g_o = v_oguess[...]
    h_u = v_rhs[0] - d_i * g_u + c * g_v
    h_v = v_rhs[1] - d_i * g_v - c * g_u
    h_o = v_orhs[...] - d_o * g_o
    own = {
        M_U: r_i * g_u,
        M_V: r_i * g_v,
        M_O: r_o * g_o,
        H_U: s_i * h_u,
        H_V: s_i * h_v,
        H_O: s_o * h_o,
        B_I: r_i * s_i,
        B_O: r_o * s_o,
        TURN: c * p_i,
    }
    for k, value in enumerate((h_u, h_v, h_o, r_i, r_o, p_i, p_o)):
        local[k] = value
    for f in range(9):
        fields[f, 0:ROWS, 0:COLS] = own[f]

    sub = iota((8, COLS), 0)
    eastward = [jnp.zeros((8, COLS), jnp.float32)] * len(TILES)
    westward = [jnp.zeros((8, COLS), jnp.float32)] * len(TILES)
    for t, f, at, n in packed_rows():
        eastward[t] = jnp.where(
            jnp.logical_and(sub >= 8 - at - n, sub < 8 - at), roll(own[f][ROWS - 8 : ROWS], -at, 0), eastward[t]
        )
        westward[t] = jnp.where(jnp.logical_and(sub >= at, sub < at + n), roll(own[f][0:8], at, 0), westward[t])
    for t in range(len(TILES)):
        zonal_out[0, t] = eastward[t]
        zonal_out[1, t] = westward[t]

    lane = iota((ROWS, 128), 1)
    halves = [jnp.zeros((ROWS, 128), jnp.float32)] * 2
    for half, f, at, n in columns():
        edge = jnp.where(lane < 64, own[f][:, 0:128], own[f][:, COLS - 128 : COLS])
        halves[half] = jnp.where(
            jnp.logical_and(lane >= at, lane < at + 2 * n), roll(edge, at + n, 1), halves[half]
        )
    turned = jnp.transpose(jnp.concatenate(halves, axis=0))[0:PACK]
    merid_out[0] = turned
    merid_out[1] = turned
    corner_out[0] = corners(turned)
    corner_out[1] = corners(turned)

    @pl.when(top)
    def _():
        step = northern_rows()
        flipped = jnp.where(
            step == 0, roll(turned, 1, 0), jnp.where(step == 1, roll(turned, 3, 0), roll(turned, 5, 0))
        )
        swap = jnp.where(
            (iota((128, 128), 0) ^ iota((128, 128), 1)) == 63, 1.0, 0.0
        ).astype(jnp.float32)
        mirrored = jnp.dot(
            flipped, swap, precision=lax.Precision.HIGHEST, preferred_element_type=jnp.float32
        )
        mirrored = jnp.where(iota((PACK, 128), 1) < 64, -mirrored, mirrored)
        merid_out[0] = mirrored
        corner_out[0] = corners(mirrored)

    @pl.when(bottom)
    def _():
        south_in[...] = jnp.zeros((STRIP, 128), jnp.float32)

    expected = len(hubs) + ngy - 1 + 2 + 3 + jnp.where(bottom, 0, 3) - jnp.where(is_hub, 1, 0)
    for k in range(3):
        expected = expected - jnp.where(mirror_self[k], 1, 0)
    for at, served in posts.items():
        expected = expected + jnp.where(jnp.logical_and(top, zz == at), len(served), 0)
    pl.semaphore_wait(barrier, expected)

    def remote(src, dst, sent, got, device):
        return pltpu.make_async_remote_copy(
            src_ref=src,
            dst_ref=dst,
            send_sem=halo_send.at[sent],
            recv_sem=halo_recv.at[got],
            device_id=device,
            device_id_type=MESH,
        )

    parts = [pl.ds(0, PACK), pl.ds(PACK, 8), pl.ds(PACK + 8, 8)]
    opposite = (0, 2, 1)
    sources = [[merid_out.at[i], corner_out.at[i], corner_out.at[i]] for i in range(2)]
    fold = [remote(sources[0][k], north_in.at[parts[k]], k, k, norths[k]) for k in range(3)]
    up = [
        remote(sources[0][k], south_in.at[parts[opposite[k]]], k, 3 + opposite[k], norths[k])
        for k in range(3)
    ]
    down = [
        remote(sources[1][k], north_in.at[parts[opposite[k]]], 3 + k, opposite[k], souths[k])
        for k in range(3)
    ]

    def to_post(k):
        post, slot = post_of(norths[k][0])
        return pltpu.make_async_remote_copy(
            src_ref=sources[0][k],
            dst_ref=post_in.at[slot, parts[k]],
            send_sem=halo_send.at[k],
            recv_sem=post_recv.at[slot],
            device_id=(post, gy),
            device_id_type=MESH,
        )

    to_east = remote(zonal_out.at[0], zonal_in.at[0], 6, 6, east)
    to_west = remote(zonal_out.at[1], zonal_in.at[1], 7, 7, west)

    target_late = [is_late(norths[k][0]) for k in range(3)]
    for k in range(3):

        @pl.when(jnp.logical_and(top, target_late[k]))
        def _():
            to_post(k).start()

        @pl.when(
            jnp.logical_and(
                jnp.logical_and(top, jnp.logical_not(target_late[k])), jnp.logical_not(mirror_self[k])
            )
        )
        def _():
            fold[k].start()

        @pl.when(mirror_self[k])
        def _():
            north_in[PACK + 8 * max(k - 1, 0) : PACK + 8 * max(k - 1, 0) + 8] = corner_out[0]

    @pl.when(jnp.logical_not(top))
    def _():
        for copy in up:
            copy.start()

    @pl.when(jnp.logical_not(bottom))
    def _():
        for copy in down:
            copy.start()

    to_east.start()
    to_west.start()

    for at, served in posts.items():

        @pl.when(jnp.logical_and(top, zz == at))
        def _():
            for slot, z in enumerate(served):
                strip = post_in.at[slot]
                pltpu.make_async_copy(strip, strip, post_recv.at[slot]).wait()
                pltpu.make_async_remote_copy(
                    src_ref=strip,
                    dst_ref=north_in,
                    send_sem=post_send.at[slot],
                    recv_sem=halo_recv.at[0],
                    device_id=(yy * nz + z, gy),
                    device_id_type=MESH,
                ).start()

    to_east.wait_recv()
    to_west.wait_recv()

    for t, f, at, n in packed_rows():
        fields[f, ROWS:EXT_ROWS, 0:COLS] = jnp.where(
            sub < 4, roll(zonal_in[1, t], -at, 0), roll(zonal_in[0, t], at, 0)
        )

    def arrived(k, dst):
        pltpu.make_async_copy(dst, dst, halo_recv.at[k]).wait()

    @pl.when(jnp.logical_and(top, late))
    def _():
        arrived(0, north_in)

    for k in range(3):

        @pl.when(jnp.logical_not(jnp.logical_or(jnp.logical_and(top, late), mirror_self[k])))
        def _():
            arrived(k, north_in.at[parts[k]])

        @pl.when(jnp.logical_not(bottom))
        def _():
            arrived(3 + k, south_in.at[parts[k]])

    northern = northern_rows() >= 0
    plane = jnp.where(northern, north_in[0:PACK], south_in[0:PACK])
    from_e, from_w = [
        jnp.where(northern, from_corners(north_in[at : at + 8]), from_corners(south_in[at : at + 8]))
        for at in (PACK, PACK + 8)
    ]
    lane = iota((PACK, 128), 1)
    pad = jnp.zeros((32 - PACK, 128), jnp.float32)
    blank = jnp.zeros((EXT_ROWS, 96), jnp.float32)
    backs = []
    for half in range(2):
        if half == 0:
            center, right, left = plane, roll(from_e, 64, 1), roll(from_w, 8, 1)
        else:
            center, right, left = roll(plane, 64, 1), from_e, roll(from_w, 72, 1)
        merged = jnp.where(lane < 64, center, jnp.where(lane < 68, right, left))
        back = jnp.transpose(jnp.concatenate([merged, pad], axis=0))[0:EXT_ROWS]
        backs.append(jnp.concatenate([back, blank], axis=1))
    for half, f, at, n in columns():
        fields[f, :, COLS:EXT_COLS] = roll(backs[half], -(at + n), 1)

    b_i = fields[B_I]
    b_o = fields[B_O]
    turn = fields[TURN]
    t_in = inner_block(turn)
    h_u, h_v, h_o = local[0], local[1], local[2]
    r_i, r_o, p_i, p_o = local[3], local[4], local[5], local[6]
    nb_u = around(fields[M_U])
    nb_v = around(fields[M_V])
    nb_o = around(fields[M_O])
    s0_u = fields[H_U] + b_i * nb_u
    s0_v = fields[H_V] + b_i * nb_v
    s0_o = fields[H_O] + b_o * nb_o
    res_u = h_u + r_i * inner_block(nb_u)
    res_v = h_v + r_i * inner_block(nb_v)
    res_o = h_o + r_o * inner_block(nb_o)
    nb_u = around(s0_u)
    nb_v = around(s0_v)
    nb_o = around(s0_o)
    s1_u = b_i * nb_u + turn * s0_v
    s1_v = b_i * nb_v - turn * s0_u
    s1_o = b_o * nb_o
    n1_u = r_i * inner_block(nb_u) + t_in * res_v
    n1_v = r_i * inner_block(nb_v) - t_in * res_u
    n1_o = r_o * inner_block(nb_o)
    n2_u = r_i * inner_block(around(s1_u)) + t_in * n1_v
    n2_v = r_i * inner_block(around(s1_v)) - t_in * n1_u
    n2_o = r_o * inner_block(around(s1_o))
    a_u, a_v, a_o = res_u - n1_u, res_v - n1_v, res_o - n1_o
    e_u, e_v, e_o = n1_u - n2_u, n1_v - n2_v, n1_o - n2_o
    z_o = p_o * res_o
    x_o = p_o * n1_o
    products = [
        a_u * a_u + a_v * a_v,
        a_u * e_u + a_v * e_v,
        e_u * e_u + e_v * e_v,
        a_u * res_u + a_v * res_v,
        e_u * res_u + e_v * res_v,
        z_o * a_o,
        x_o * a_o,
        x_o * e_o,
        z_o * res_o,
        x_o * res_o,
    ]
    local[0] = p_i * res_u
    local[1] = p_i * res_v
    local[2] = z_o
    local[3] = p_i * n1_u
    local[4] = p_i * n1_v
    local[5] = x_o

    row = iota((16, 128), 0)
    sums = jnp.zeros((16, 128), jnp.float32)
    for k, product in enumerate(products):
        half = product[:, 0:128] + product[:, 128:256]
        sums = jnp.where(row == k, jnp.sum(half, axis=0, keepdims=True), sums)
    sums = jnp.sum(sums, axis=1, keepdims=True)
    mine = jnp.sum(jnp.where(row == iota((16, 128), 1), sums, 0.0), axis=0, keepdims=True)

    def rows_of(slots, count, sem):
        return pltpu.make_async_copy(slots.at[pl.ds(0, count)], slots.at[pl.ds(0, count)], sem)

    def send_row(slots, at, dst, dst_at, send, recv, device):
        pltpu.make_async_remote_copy(
            src_ref=slots.at[at],
            dst_ref=dst.at[dst_at],
            send_sem=sum_sems.at[send],
            recv_sem=sum_sems.at[recv],
            device_id=device,
            device_id_type=MESH,
        ).start()

    sum_gy[gy] = mine
    for p in gy_peers:
        send_row(sum_gy, gy, sum_gy, gy, 0, 1, (gx, p))
    rows_of(sum_gy, ngy - 1, sum_sems.at[1]).wait()
    total = sum_gy[0]
    for k in range(1, ngy):
        total = total + sum_gy[k]

    sum_plane[gx] = total
    for hub in hubs:

        @pl.when(gx != hub)
        def _():
            send_row(sum_plane, gx, sum_plane, gx, 2, 3, (hub, gy))

    @pl.when(is_hub)
    def _():
        rows_of(sum_plane, ngx - 1, sum_sems.at[3]).wait()
        parts_of = [sum_plane[k] for k in range(8)]
        for k in range(8, ngx):
            parts_of[k % 8] = parts_of[k % 8] + sum_plane[k]
        while len(parts_of) > 1:
            parts_of = [a + b for a, b in zip(parts_of[0::2], parts_of[1::2])]
        whole = parts_of[0]
        result[0] = whole
        result[1] = whole
        for z in later:

            @pl.when(zz == nhub - 1)
            def _():
                send_row(result, 0, result, 1, 4, 5, (yy * nz + z, gy))

    @pl.when(jnp.logical_not(is_hub))
    def _():
        rows_of(result, 1, sum_sems.at[5]).wait()

    total = result[1]

    def item(k):
        return total[0:1, k : k + 1]

    def solve(k11, k12, k22, k1, k2):
        scale = 1.0 / item(k11)
        a12, a22 = item(k12) * scale, item(k22) * scale
        f1, f2 = item(k1) * scale, item(k2) * scale
        det = 1.0 / (a22 - a12 * a12)
        return (a22 * f1 - a12 * f2) * det, (f2 - a12 * f1) * det

    c1, c2 = solve(0, 1, 2, 3, 4)
    d1, d2 = solve(5, 6, 7, 8, 9)
    velocity[0] = v_guess[0] + c1 * local[0] + c2 * local[3]
    velocity[1] = v_guess[1] + c1 * local[1] + c2 * local[4]
    level[...] = v_oguess[...] + d1 * local[2] + d2 * local[5]

    for k in range(3):

        @pl.when(jnp.logical_and(top, jnp.logical_not(mirror_self[k])))
        def _():
            fold[k].wait_send()

    for at, served in posts.items():

        @pl.when(jnp.logical_and(top, zz == at))
        def _():
            for slot, _ in enumerate(served):
                pltpu.make_async_copy(post_in.at[slot], post_in.at[slot], post_send.at[slot]).wait()

    @pl.when(jnp.logical_not(top))
    def _():
        for copy in up:
            copy.wait_send()

    @pl.when(jnp.logical_not(bottom))
    def _():
        for k in range(3):
            down[k].wait_send()

    to_east.wait_send()
    to_west.wait_send()
    rows_of(sum_gy, ngy - 1, sum_sems.at[0]).wait()

    @pl.when(is_hub)
    def _():
        rows_of(sum_plane, len(hubs) - 1, sum_sems.at[2]).wait()

    @pl.when(jnp.logical_not(is_hub))
    def _():
        rows_of(sum_plane, len(hubs), sum_sems.at[2]).wait()

    @pl.when(zz == nhub - 1)
    def _():
        rows_of(sum_plane, len(later), sum_sems.at[4]).wait()


def put_out(velocity, level, velocity_out, level_out, sems):
    copies = [
        pltpu.make_async_copy(velocity, velocity_out, sems.at[0]),
        pltpu.make_async_copy(level, level_out, sems.at[1]),
    ]
    for copy in copies:
        copy.start()
    for copy in copies:
        copy.wait()


def build(mesh, ny, nz, interpret=False):
    ngy = mesh.shape["gy"]
    f32 = jnp.float32
    block = pltpu.VMEM((ROWS, COLS), f32)
    pair = pltpu.VMEM((2, ROWS, COLS), f32)
    whole = pltpu.VMEM((ROWS, COLS), jnp.int32)
    dma = pltpu.SemaphoreType.DMA

    def body(*args):
        solved = pl.pallas_call(
            functools.partial(kernel, (ny, nz, ngy)),
            out_shape=(
                pltpu.VMEM((2, ROWS, COLS), f32),
                pltpu.VMEM((ROWS, COLS), f32),
            ),
            in_specs=[pl.BlockSpec(memory_space=pl.ANY)] * 10,
            out_specs=(pl.BlockSpec(memory_space=pltpu.VMEM), pl.BlockSpec(memory_space=pltpu.VMEM)),
            scratch_shapes=[
                pair,
                pair,
                block,
                block,
                block,
                block,
                block,
                block,
                whole,
                whole,
                pltpu.VMEM((9, EXT_ROWS, EXT_COLS), f32),
                pltpu.VMEM((7, ROWS, COLS), f32),
                pltpu.VMEM((2, 3, 8, COLS), f32),
                pltpu.VMEM((2, 3, 8, COLS), f32),
                pltpu.VMEM((2, PACK, 128), f32),
                pltpu.VMEM((2, 8, 128), f32),
                pltpu.VMEM((STRIP, 128), f32),
                pltpu.VMEM((STRIP, 128), f32),
                pltpu.VMEM((nz - 2 * nz // 3, STRIP, 128), f32),
                pltpu.VMEM((ngy, 1, 128), f32),
                pltpu.VMEM((ny * nz, 1, 128), f32),
                pltpu.VMEM((2, 1, 128), f32),
                dma((10,)),
                dma((8,)),
                dma((8,)),
                dma((nz - 2 * nz // 3,)),
                dma((nz - 2 * nz // 3,)),
                dma((6,)),
            ],
            compiler_params=pltpu.CompilerParams(collective_id=0, has_side_effects=True, vmem_limit_bytes=16 * 1024 * 1024),
            name="picard",
        )(*[pltpu.with_memory_space_constraint(a, pltpu.HBM) for a in args])
        return pl.pallas_call(
            put_out,
            out_shape=(pltpu.HBM((2, ROWS, COLS), f32), pltpu.HBM((ROWS, COLS), f32)),
            in_specs=[pl.BlockSpec(memory_space=pltpu.VMEM)] * 2,
            out_specs=(pl.BlockSpec(memory_space=pltpu.HBM), pl.BlockSpec(memory_space=pltpu.HBM)),
            scratch_shapes=[dma((2,))],
            compiler_params=pltpu.CompilerParams(vmem_limit_bytes=4 * 1024 * 1024),
            name="put_out",
        )(*[pltpu.with_memory_space_constraint(a, pltpu.VMEM) for a in solved])

    both = P(None, "gx", "gy")
    one = P("gx", "gy")
    return jax.shard_map(
        body,
        mesh=mesh,
        in_specs=(both, both, one, one, one, one, one, one, one, one),
        out_specs=(both, one),
        check_vma=False,
    )


def solution(mesh):
    return build(mesh, 8, 12)
```
